256 devices in a mesh: frame: 32 (over x, z_hi, core), coil: 8 (over z_lo, y).
Axes of the slice: x: 4, y: 4, z: 8 (z_hi: 4, z_lo: 2; z = z_hi * 2 + z_lo), core: 2. Of those that a mesh axis runs over, the one named last changes fastest.
Arguments:
- kspace: bfloat16 [32, 64, 256, 512], P('frame', 'coil'), may hold values from -6 to 6
- sens: bfloat16 [64, 256, 512], P('coil'), may hold values from -0.5 to 0.5
- mask: int32 [32, 64, 256], P('frame', 'coil'), may hold values 0 or 1
- image: float32 [32, 256, 512], P('frame', 'coil'), may hold values from -6 to 6
- w_first: bfloat16 [3, 3, 3, 64, 2], replicated, may hold values from -0.875 to 0.875
- b_first: float32 [64], replicated, may hold values from -3 to 3
- w_mid: bfloat16 [3, 3, 3, 64, 64], replicated, may hold values from -0.15625 to 0.15625
- b_mid: float32 [64], replicated, may hold values from -3 to 3
- w_last: bfloat16 [3, 3, 3, 2, 64], replicated, may hold values from -0.15625 to 0.15625
Outputs:
- recon: float32 [32, 256, 512], P('frame', 'coil')
The draws below stay inside these ranges and needn't reach their ends.
Inputs may be any that keep to these rules, and one draw needn't show every extreme that they name: mask is 1 on the acquired phase-encoding lines of a frame and coil and 0 on the others.
All inputs are finite; a program needn't handle non-finite values. No bound on the sum of `mask` on one device may be relied on, other than what follows from the above.
Results may differ from the reference program's by a relative error of at most 0.006.
Values may be sent and summed in bfloat16 or wider, within the bound.
A program may use at most 64 MiB of HBM per device.

```python
import math
import jax
import jax.numpy as jnp
from jax import lax

NR = 256
NC = 256
COILS = 64
CH = 64
OUTER = 1
DSTEPS = 1
FRAMES = 32


def place_ends(values, key, least, largest):
    extent = values.shape
    spot = [jax.random.randint(jax.random.fold_in(key, axis), (), 0, extent[axis]) for axis in range(len(extent))]
    values = values.at[tuple(spot)].set(least)
    longest = extent.index(max(extent))
    spot[longest] = (spot[longest] + 1) % extent[longest]
    return values.at[tuple(spot)].set(largest)


def levels(rng, extent, pieces, smallest, top_value):
    factor_of = 1.0
    for dim, parts in pieces:
        draws = jax.random.uniform(jax.random.fold_in(jax.random.fold_in(rng, 6), dim), (parts,), jnp.float32, smallest / len(pieces), top_value / len(pieces))
        factor_of = factor_of * jnp.repeat(jnp.exp(draws), extent[dim] // parts).reshape((-1,) + (1,) * (len(extent) - 1 - dim))
    return factor_of


def scatter_about(rng, dims, width, reach, pieces=(), held_as=jnp.bfloat16):
    loudness = levels(rng, dims, pieces, -0.22, 0.18) if pieces else 1.0
    values = jax.random.normal(rng, dims, jnp.float32) * width * loudness
    return jnp.minimum(jnp.maximum(values, -reach), reach).astype(held_as)


def setup_inputs(seed: int = 0) -> dict:
    key_of = jax.random.split(jax.random.key(seed), 10)
    return {
        "kspace": scatter_about(key_of[0], (FRAMES, COILS, NR, 2 * NC), 1.0, 6.0, ((0, 32), (1, 8))),
        "sens": scatter_about(key_of[1], (COILS, NR, 2 * NC), (2 * COILS) ** -0.5, 0.5, ((0, 8),)),
        "mask": place_ends((jax.random.randint(key_of[2], (FRAMES, COILS, NR), 0, 3) < 1).astype(jnp.int32), jax.random.fold_in(key_of[2], 1), 0, 1),
        "image": scatter_about(key_of[3], (FRAMES, NR, 2 * NC), 1.0, 6.0, ((0, 32), (1, 8)), jnp.float32),
        "w_first": scatter_about(key_of[4], (3, 3, 3, CH, 2), 54 ** -0.5, 0.875),
        "b_first": scatter_about(key_of[5], (CH,), 0.5, 3.0, (), jnp.float32),
        "w_mid": scatter_about(key_of[6], (3, 3, 3, CH, CH), (27 * CH) ** -0.5, 0.15625),
        "b_mid": scatter_about(key_of[7], (CH,), 0.5, 3.0, (), jnp.float32),
        "w_last": scatter_about(key_of[8], (3, 3, 3, 2, CH), (27 * CH) ** -0.5, 0.15625),
    }


step_size = 1.0

def dft_parts(order):
    indices = jnp.arange(order, dtype=jnp.int32)
    phases = indices[:, None] * indices[None, :] % order
    angles = phases.astype(jnp.float32) * (2.0 * math.pi / order)
    factor = 1.0 / math.sqrt(order)
    return ((jnp.cos(angles) * factor).astype(jnp.bfloat16), (-jnp.sin(angles) * factor).astype(jnp.bfloat16))

def column_tables(real_part, imag_part):
    ahead = jnp.concatenate([jnp.concatenate([real_part, imag_part], 1), jnp.concatenate([-imag_part, real_part], 1)], 0)
    behind = jnp.concatenate([jnp.concatenate([real_part, -imag_part], 1), jnp.concatenate([imag_part, real_part], 1)], 0)
    return (ahead, behind)

def swapped(values):
    half_width = values.shape[-1] // 2
    return jnp.concatenate([-values[..., half_width:], values[..., :half_width]], -1)

def complex_mul(first, second):
    half_width = first.shape[-1] // 2
    first_re, first_im = (first[..., :half_width], first[..., half_width:])
    second_re, second_im = (second[..., :half_width], second[..., half_width:])
    return jnp.concatenate([first_re * second_re - first_im * second_im, first_re * second_im + first_im * second_re], -1)

def conj_mul(first, second):
    half_width = first.shape[-1] // 2
    first_re, first_im = (first[..., :half_width], first[..., half_width:])
    second_re, second_im = (second[..., :half_width], second[..., half_width:])
    return jnp.concatenate([first_re * second_re + first_im * second_im, first_re * second_im - first_im * second_re], -1)

def data_frame(image_now, kspace, sampled, sens, row_real, row_imag, ahead, behind):
    f32 = jnp.float32
    image_low = image_now.astype(jnp.bfloat16)
    coil_image = complex_mul(sens.astype(f32), image_low.astype(f32)[None]).astype(jnp.bfloat16)
    cols_spectrum = jnp.einsum('crm,mn->crn', coil_image.astype(f32), ahead.astype(f32)).astype(jnp.bfloat16)
    row_ahead = jnp.concatenate([row_real, row_imag], 1)
    stacked = jnp.concatenate([cols_spectrum, swapped(cols_spectrum)], 1)
    estimate = jnp.einsum('kr,crn->ckn', row_ahead.astype(f32), stacked.astype(f32))
    misfit = (sampled.astype(f32)[..., None] * (estimate - kspace.astype(f32))).astype(jnp.bfloat16)
    back_cols = jnp.einsum('ckm,mn->ckn', misfit.astype(f32), behind.astype(f32)).astype(jnp.bfloat16)
    row_behind = jnp.concatenate([row_real, -row_imag], 1)
    stacked_back = jnp.concatenate([back_cols, swapped(back_cols)], 1)
    back_image = jnp.einsum('rk,ckn->crn', row_behind.astype(f32), stacked_back.astype(f32))
    gradient = lax.optimization_barrier(jnp.sum(conj_mul(sens.astype(f32), back_image), 0))
    return image_now - step_size * gradient

def conv_layer(padded, weight):
    frames = padded.shape[0] - 2
    rows = padded.shape[1] - 2
    out_chan = weight.shape[3]
    in_chan = weight.shape[4]
    window = jnp.concatenate([padded[tap_frame:tap_frame + frames, tap_row:tap_row + rows] for tap_frame in range(3) for tap_row in range(3)], 2)
    matrix = jnp.transpose(weight, (2, 3, 0, 1, 4)).reshape(3 * out_chan, 9 * in_chan)
    taps_out = jnp.einsum('km,frmn->frkn', matrix.astype(jnp.float32), window.astype(jnp.float32))
    left_taps = taps_out[:, :, :out_chan]
    centre = taps_out[:, :, out_chan:2 * out_chan]
    right_taps = taps_out[:, :, 2 * out_chan:]
    zeros_col = jnp.zeros_like(left_taps[..., :1])
    return centre + jnp.concatenate([zeros_col, left_taps[..., :-1]], -1) + jnp.concatenate([right_taps[..., 1:], zeros_col], -1)

def conv_frames(hidden, weight):
    padded = jnp.pad(hidden, ((1, 1), (1, 1), (0, 0), (0, 0)))

    def one_frame(frame_idx):
        block = lax.dynamic_slice_in_dim(padded, frame_idx, 3, 0)
        return conv_layer(block, weight)[0]
    return lax.map(one_frame, jnp.arange(hidden.shape[0], dtype=jnp.int32))

def denoise(image_now, w_first, b_first, w_mid, b_mid, w_last):
    frames, rows, double = image_now.shape
    hidden = image_now.reshape(frames, rows, 2, double // 2).astype(jnp.bfloat16)
    first = jax.nn.relu(conv_frames(hidden, w_first) + b_first[None, None, :, None]).astype(jnp.bfloat16)
    second = jax.nn.relu(conv_frames(first, w_mid) + b_mid[None, None, :, None]).astype(jnp.bfloat16)
    update = conv_frames(second, w_last)
    return image_now + update.reshape(frames, rows, double)

def reference(kspace, sens, mask, image, w_first, b_first, w_mid, b_mid, w_last):
    row_real, row_imag = dft_parts(sens.shape[1])
    col_real, col_imag = dft_parts(sens.shape[2] // 2)
    ahead, behind = column_tables(col_real, col_imag)
    image_now = image
    for sweep_idx in range(OUTER):
        for inner_idx in range(DSTEPS):
            image_now = lax.map(lambda items: data_frame(items[0], items[1], items[2], sens, row_real, row_imag, ahead, behind), (image_now, kspace, mask))
        image_now = denoise(image_now, w_first, b_first, w_mid, b_mid, w_last)
    return image_now
```

```python
import functools

import jax
import jax.numpy as jnp
import numpy as np
from jax import lax
from jax.experimental import pallas as pl
from jax.experimental.pallas import tpu as pltpu
from jax.sharding import PartitionSpec as P

F32 = jnp.float32
BF16 = jnp.bfloat16
MESH = pl.DeviceIdType.MESH

ROWS = 256
N = 256
RB = 32
HR = 48
NCO = 8
CH = 64
GRP = 8


def dft_tables():
    idx = np.arange(N)
    ang = (idx[:, None] * idx[None, :] % N) * (2.0 * np.pi / N)
    fr = (np.cos(ang) / np.sqrt(N)).astype(np.float32)
    fi = (-np.sin(ang) / np.sqrt(N)).astype(np.float32)
    cols = np.block([[fr, fi], [-fi, fr]])
    back = np.block([[fr, -fi], [fi, fr]])
    rows = np.block([[fr, -fi], [fi, fr]])
    rback = np.block([[fr, fi], [-fi, fr]])
    return cols, back, rows, rback


def shift_right(v):
    lane = lax.broadcasted_iota(jnp.int32, v.shape, 1)
    return jnp.where(lane == 0, 0.0, pltpu.roll(v, 1, axis=1))


def shift_left(v):
    lane = lax.broadcasted_iota(jnp.int32, v.shape, 1)
    return jnp.where(lane == N - 1, 0.0, pltpu.roll(v, N - 1, axis=1))


def dot(a, b):
    return jnp.dot(a, b, preferred_element_type=F32)


def kernel(
    frames,
    kspace_hbm, sens_hbm, mask_hbm, image_hbm, ta_hbm, tb_hbm, w1_hbm, w2_hbm, w3_hbm, b1_hbm, b2_hbm,
    out_ref,
    ksp, sens, mask, image, ta, tb, w1, w2, w3, b1, b2,
    xb, ci, cols, acc, gs, grecv, xr, x48, hb, kb, h1, h2, psend, precv,
    lsem, asend, arecv, bsend, brecv, csend, crecv, dsend, drecv,
):
    t = lax.axis_index("frame")
    j = lax.axis_index("coil")
    r0 = pl.multiple_of(j * RB, RB)

    loads = [
        pltpu.make_async_copy(src, dst, lsem.at[i])
        for i, (src, dst) in enumerate(
            [
                (image_hbm, image), (sens_hbm, sens), (ta_hbm, ta), (tb_hbm, tb), (kspace_hbm, ksp),
                (mask_hbm, mask), (w1_hbm, w1), (w2_hbm, w2), (w3_hbm, w3), (b1_hbm, b1), (b2_hbm, b2),
            ]
        )
    ]
    for c in loads:
        c.start()

    partners = [(d, (t + d >= 0) & (t + d < frames)) for d in (-2, -1, 1, 2)]

    barrier = pltpu.get_barrier_semaphore()
    for s in range(1, GRP):
        pl.semaphore_signal(barrier, inc=1, device_id={"coil": lax.rem(j + s, GRP)}, device_id_type=MESH)
    for d, here in partners:
        @pl.when(here)
        def _():
            pl.semaphore_signal(barrier, inc=1, device_id={"frame": t + d}, device_id_type=MESH)

    loads[0].wait()
    xb[pl.ds(r0, RB), :] = image[...].astype(BF16)
    present = sum(here.astype(jnp.int32) for _, here in partners)
    pl.semaphore_wait(barrier, GRP - 1 + present)

    acopy = []
    for s in range(1, GRP):
        c = pltpu.make_async_remote_copy(
            src_ref=xb.at[pl.ds(r0, RB)],
            dst_ref=xb.at[pl.ds(r0, RB)],
            send_sem=asend.at[s],
            recv_sem=arecv.at[s],
            device_id={"coil": lax.rem(j + s, GRP)},
            device_id_type=MESH,
        )
        c.start()
        acopy.append(c)

    loads[1].wait()
    loads[2].wait()

    def columns(q):
        rq = pl.multiple_of(q * RB, RB)
        xv = xb[pl.ds(rq, RB), :].astype(F32)
        x_re, x_im = xv[:, :N], xv[:, N:]
        for c in range(NCO):
            sv = sens[c, pl.ds(rq, RB), :].astype(F32)
            s_re, s_im = sv[:, :N], sv[:, N:]
            ci[c * RB : (c + 1) * RB, :N] = (s_re * x_re - s_im * x_im).astype(BF16)
            ci[c * RB : (c + 1) * RB, N:] = (s_re * x_im + s_im * x_re).astype(BF16)
        for half in range(2):
            spec = dot(ci[...], ta[0, :, half * N : (half + 1) * N]).astype(BF16)
            for c in range(NCO):
                cols[c, pl.ds(half * ROWS + rq, RB), :] = spec[c * RB : (c + 1) * RB]

    columns(j)

    @pl.loop(1, GRP)
    def _(s):
        pltpu.make_async_remote_copy(
            src_ref=xb.at[pl.ds(r0, RB)],
            dst_ref=xb.at[pl.ds(pl.multiple_of(lax.rem(j - s + GRP, GRP) * RB, RB), RB)],
            send_sem=asend.at[s],
            recv_sem=arecv.at[s],
            device_id={"coil": lax.rem(j + s, GRP)},
            device_id_type=MESH,
        ).wait_recv()
        columns(lax.rem(j - s + GRP, GRP))

    loads[3].wait()
    loads[4].wait()
    loads[5].wait()

    def coil(c):
        halves = []
        for half in range(2):
            est = dot(tb[0, half * ROWS : (half + 1) * ROWS, :], cols[c])
            k = ksp[c, :, half * N : (half + 1) * N].astype(F32)
            halves.append((est - k).astype(BF16))
        misfit = jnp.concatenate(halves, axis=1)
        stacked = jnp.concatenate(
            [dot(misfit, ta[1, :, half * N : (half + 1) * N]).astype(BF16) for half in range(2)], axis=0
        )
        m = mask[pl.ds(c, 1), :].astype(F32).astype(BF16)
        mm = jnp.concatenate([m, m], axis=1)
        b_re = dot(tb[1, :ROWS, :] * mm, stacked)
        b_im = dot(tb[1, ROWS:, :] * mm, stacked)
        s_re, s_im = sens[c, :, :N].astype(F32), sens[c, :, N:].astype(F32)
        return s_re * b_re + s_im * b_im, s_re * b_im - s_im * b_re

    first_re, first_im = coil(0)
    acc[:, :N] = first_re
    acc[:, N:] = first_im

    @pl.loop(1, NCO)
    def _(c):
        g_re, g_im = coil(c)
        acc[:, :N] += g_re
        acc[:, N:] += g_im

    gs[:ROWS, :] = pltpu.roll(acc[...], 3, axis=0).astype(BF16)
    gs[ROWS : ROWS + 16, :] = pltpu.roll(acc[ROWS - 16 :, :], 3, axis=0).astype(BF16)

    bcopy = []
    for s in range(1, GRP):
        to = lax.rem(j + s, GRP)
        c = pltpu.make_async_remote_copy(
            src_ref=gs.at[pl.ds(pl.multiple_of(to * RB, RB), HR)],
            dst_ref=grecv.at[s],
            send_sem=bsend.at[s],
            recv_sem=brecv.at[s],
            device_id={"coil": to},
            device_id_type=MESH,
        )
        c.start()
        bcopy.append(c)

    xr[:ROWS, :] = pltpu.roll(xb[...].astype(F32), 3, axis=0)
    xr[ROWS : ROWS + 16, :] = jnp.zeros((16, 2 * N), F32)
    x48[...] = xr[pl.ds(r0, HR), :]
    x48[3 : 3 + RB, :] = image[...]
    for c in loads[6:]:
        c.wait()
    total = x48[...] - gs[pl.ds(r0, HR), :].astype(F32)
    for c in bcopy:
        c.wait_recv()
    for s in range(1, GRP):
        total = total - grecv[s].astype(F32)
    row = r0 - 3 + lax.broadcasted_iota(jnp.int32, (HR, 2 * N), 0)
    total = jnp.where((row >= 0) & (row < ROWS), total, 0.0)
    x48[...] = total
    hb[2] = total.astype(BF16)

    for d, here in partners:
        def ccopy(d=d):
            return pltpu.make_async_remote_copy(
                src_ref=hb.at[2],
                dst_ref=hb.at[2 - d],
                send_sem=csend.at[d + 2],
                recv_sem=crecv.at[d + 2],
                device_id={"frame": t + d},
                device_id_type=MESH,
            )

        @pl.when(here)
        def _():
            ccopy().start()

        @pl.when(jnp.logical_not(here))
        def _():
            hb[2 + d] = jnp.zeros((HR, 2 * N), BF16)

    def planes(f):
        v = hb[f].astype(F32)
        parts = []
        for half in range(2):
            p = v[:, half * N : (half + 1) * N]
            parts += [shift_right(p), p, shift_left(p)]
        for i in range(HR // 8):
            kb[i, f * HR : (f + 1) * HR, :] = jnp.concatenate(
                [p[8 * i : 8 * i + 8] for p in parts], axis=0
            ).astype(BF16)

    planes(2)
    for d, here in partners:
        @pl.when(here)
        def _():
            pltpu.make_async_remote_copy(
                src_ref=hb.at[2],
                dst_ref=hb.at[2 + d],
                send_sem=csend.at[2 - d],
                recv_sem=crecv.at[2 - d],
                device_id={"frame": t + d},
                device_id_type=MESH,
            ).wait_recv()

        planes(2 + d)

    bias1 = b1[...]
    for f in range(3):
        @pl.loop(0, 5)
        def _(i):
            here_k = kb[i, f * HR : (f + 3) * HR, :]
            next_k = kb[i + 1, f * HR : (f + 3) * HR, :]
            top = dot(w1[:384, :], here_k)
            low = dot(w1[384:512, :], here_k) + dot(w1[512:, :], next_k)
            base = pl.multiple_of(i * 512, 512)
            for q in range(6):
                h1[f, pl.ds(base + q * CH, CH), :] = jnp.maximum(top[q * CH : (q + 1) * CH] + bias1, 0.0).astype(BF16)
            for q in range(2):
                h1[f, pl.ds(base + (6 + q) * CH, CH), :] = jnp.maximum(low[q * CH : (q + 1) * CH] + bias1, 0.0).astype(BF16)

    @pl.when(j == 0)
    def _():
        h1[:, : 2 * CH, :] = jnp.zeros((3, 2 * CH, N), BF16)

    @pl.when(j == GRP - 1)
    def _():
        h1[:, 34 * CH :, :] = jnp.zeros((3, 6 * CH, N), BF16)

    @pl.when(t == 0)
    def _():
        h1[0] = jnp.zeros((40 * CH, N), BF16)

    @pl.when(t == frames - 1)
    def _():
        h1[2] = jnp.zeros((40 * CH, N), BF16)

    bias2 = b2[...]

    @pl.loop(0, 17)
    def _(i):
        for q in range(2):
            base = pl.multiple_of((2 * i + q) * CH, CH)
            taps = dot(w2[0], h1[0, pl.ds(base, 3 * CH), :])
            taps += dot(w2[1], h1[1, pl.ds(base, 3 * CH), :])
            taps += dot(w2[2], h1[2, pl.ds(base, 3 * CH), :])
            v = taps[CH : 2 * CH] + shift_right(taps[:CH]) + shift_left(taps[2 * CH :]) + bias2
            h2[pl.ds(base, CH), :] = jnp.maximum(v, 0.0).astype(BF16)

    @pl.when(j == 0)
    def _():
        h2[:CH, :] = jnp.zeros((CH, N), BF16)

    @pl.when(j == GRP - 1)
    def _():
        h2[33 * CH :, :] = jnp.zeros((CH, N), BF16)

    @pl.loop(0, RB // 8)
    def _(i):
        base = pl.multiple_of(i * 8 * CH, 8 * CH)
        taps = dot(w3[...], h2[pl.ds(base, 10 * CH), :])
        v = taps[48:96] + shift_right(taps[:48]) + shift_left(taps[96:])
        ri = pl.multiple_of(i * 8, 8)
        for a in range(3):
            for half in range(2):
                o = (a * 2 + half) * 8
                psend[a, pl.ds(ri, 8), half * N : (half + 1) * N] = v[o : o + 8]

    ends = [(1, 0, t + 1 < frames), (-1, 2, t >= 1)]
    for n, (d, a, here) in enumerate(ends):
        @pl.when(here)
        def _():
            pltpu.make_async_remote_copy(
                src_ref=psend.at[a],
                dst_ref=precv.at[n],
                send_sem=dsend.at[n],
                recv_sem=drecv.at[n],
                device_id={"frame": t + d},
                device_id_type=MESH,
            ).start()

    out_ref[...] = x48[3 : 3 + RB, :] + psend[1]
    for n, (d, a, here) in enumerate(ends):
        @pl.when((t - d >= 0) & (t - d < frames))
        def _():
            pltpu.make_async_remote_copy(
                src_ref=psend.at[a],
                dst_ref=precv.at[n],
                send_sem=dsend.at[n],
                recv_sem=drecv.at[n],
                device_id={"frame": t - d},
                device_id_type=MESH,
            ).wait_recv()
            out_ref[...] += precv[n]

    for c in acopy + bcopy:
        c.wait_send()
    for d, here in partners:
        @pl.when(here)
        def _():
            pltpu.make_async_remote_copy(
                src_ref=hb.at[2],
                dst_ref=hb.at[2 - d],
                send_sem=csend.at[d + 2],
                recv_sem=crecv.at[d + 2],
                device_id={"frame": t + d},
                device_id_type=MESH,
            ).wait_send()
    for n, (d, a, here) in enumerate(ends):
        @pl.when(here)
        def _():
            pltpu.make_async_remote_copy(
                src_ref=psend.at[a],
                dst_ref=precv.at[n],
                send_sem=dsend.at[n],
                recv_sem=drecv.at[n],
                device_id={"frame": t + d},
                device_id_type=MESH,
            ).wait_send()


def spread(rows, width, first):
    out = np.zeros((3, rows, width), np.float32)
    for q in range(rows):
        for b in range(3):
            u = q + first + b
            if 0 <= u < width:
                out[b, q, u] = 1
    return out


def shards(frames, kspace, sens, mask, image, w_first, b_first, w_mid, b_mid, w_last):
    cols, back, rows, rback = dft_tables()
    ta = jnp.asarray(np.stack([cols, back]), BF16)
    tb = jnp.asarray(np.stack([rows, rback]), BF16)
    here = spread(8, 8, 0)
    ahead = spread(2, 8, -2)
    pick1 = jnp.asarray(np.concatenate([here, ahead], axis=1), BF16)
    w1 = jnp.einsum("abeoc,bqu->qoaceu", w_first, pick1).reshape(10 * CH, 3 * HR)
    w2 = jnp.transpose(w_mid, (0, 2, 3, 1, 4)).reshape(3, 3 * CH, 3 * CH)
    pick3 = jnp.asarray(spread(8, 10, 0), BF16)
    w3 = jnp.einsum("abeoi,bqu->eaoqui", w_last, pick3).reshape(144, 10 * CH)
    b1 = jnp.broadcast_to(b_first[:, None], (CH, N))
    b2 = jnp.broadcast_to(b_mid[:, None], (CH, N))
    args = (kspace[0], sens, mask[0], image[0], ta, tb, w1, w2, w3, b1, b2)
    order = args
    dma = pltpu.SemaphoreType.DMA
    out = pl.pallas_call(
        functools.partial(kernel, frames),
        out_shape=jax.ShapeDtypeStruct((RB, 2 * N), F32),
        in_specs=[pl.BlockSpec(memory_space=pl.ANY)] * len(args),
        out_specs=pl.BlockSpec(memory_space=pltpu.VMEM),
        scratch_shapes=[pltpu.VMEM(a.shape, a.dtype) for a in order]
        + [
            pltpu.VMEM((ROWS, 2 * N), BF16),
            pltpu.VMEM((NCO * RB, 2 * N), BF16),
            pltpu.VMEM((NCO, 2 * ROWS, N), BF16),
            pltpu.VMEM((ROWS, 2 * N), F32),
            pltpu.VMEM((ROWS + 16, 2 * N), BF16),
            pltpu.VMEM((GRP, HR, 2 * N), BF16),
            pltpu.VMEM((ROWS + 16, 2 * N), F32),
            pltpu.VMEM((HR, 2 * N), F32),
            pltpu.VMEM((5, HR, 2 * N), BF16),
            pltpu.VMEM((HR // 8, 5 * HR, N), BF16),
            pltpu.VMEM((3, 40 * CH, N), BF16),
            pltpu.VMEM((34 * CH, N), BF16),
            pltpu.VMEM((3, RB, 2 * N), F32),
            pltpu.VMEM((2, RB, 2 * N), F32),
            dma((len(args),)), dma((GRP,)), dma((GRP,)), dma((GRP,)), dma((GRP,)),
            dma((5,)), dma((5,)), dma((2,)), dma((2,)),
        ],
        compiler_params=pltpu.CompilerParams(
            collective_id=0, has_side_effects=True, vmem_limit_bytes=56 * 1024 * 1024
        ),
    )(*args)
    return out[None]


def solution(mesh):
    in_specs = (
        P("frame", "coil", None, None),
        P("coil", None, None),
        P("frame", "coil", None),
        P("frame", "coil", None),
        P(),
        P(),
        P(),
        P(),
        P(),
    )
    out_specs = P("frame", "coil", None)
    body = functools.partial(shards, mesh.shape["frame"])
    return jax.shard_map(body, mesh=mesh, in_specs=in_specs, out_specs=out_specs, check_vma=False)
```

```python
import functools

import jax
import jax.numpy as jnp
import numpy as np
from jax import lax
from jax.experimental import pallas as pl
from jax.experimental.pallas import tpu as pltpu
from jax.sharding import PartitionSpec as P

F32 = jnp.float32
BF16 = jnp.bfloat16
MESH = pl.DeviceIdType.MESH

ROWS = 256
N = 256
RB = 32
HR = 48
NCO = 8
CH = 64
GRP = 8


def dft_tables():
    idx = np.arange(N)
    ang = (idx[:, None] * idx[None, :] % N) * (2.0 * np.pi / N)
    fr = (np.cos(ang) / np.sqrt(N)).astype(np.float32)
    fi = (-np.sin(ang) / np.sqrt(N)).astype(np.float32)
    cols = np.block([[fr, fi], [-fi, fr]])
    back = np.block([[fr, -fi], [fi, fr]])
    rows = np.block([[fr, -fi], [fi, fr]])
    rback = np.block([[fr, fi], [-fi, fr]])
    return cols, back, rows, rback


def shift_right(v):
    lane = lax.broadcasted_iota(jnp.int32, v.shape, 1)
    return jnp.where(lane == 0, 0.0, pltpu.roll(v, 1, axis=1))


def shift_left(v):
    lane = lax.broadcasted_iota(jnp.int32, v.shape, 1)
    return jnp.where(lane == N - 1, 0.0, pltpu.roll(v, N - 1, axis=1))


def dot(a, b):
    return jnp.dot(a, b, preferred_element_type=F32)


def kernel(
    frames,
    kspace_hbm, sens_hbm, mask_hbm, image_hbm, ta_hbm, tb_hbm, w1_hbm, w2_hbm, w3_hbm, b1_hbm, b2_hbm,
    out_ref,
    ksp, sens, mask, image, ta, tb, w1, w2, w3, b1, b2,
    xb, ci, cols, misfit, stacked, acc, gs, grecv, xr, x48, hb, kb, h1, h2, psend, precv,
    lsem, asend, arecv, bsend, brecv, csend, crecv, dsend, drecv,
):
    t = lax.axis_index("frame")
    j = lax.axis_index("coil")
    r0 = pl.multiple_of(j * RB, RB)

    loads = [
        pltpu.make_async_copy(src, dst, lsem.at[i])
        for i, (src, dst) in enumerate(
            [
                (image_hbm, image), (sens_hbm, sens), (ta_hbm, ta), (tb_hbm, tb), (kspace_hbm, ksp),
                (mask_hbm, mask), (w1_hbm, w1), (w2_hbm, w2), (w3_hbm, w3), (b1_hbm, b1), (b2_hbm, b2),
            ]
        )
    ]
    for c in loads:
        c.start()

    partners = [(d, (t + d >= 0) & (t + d < frames)) for d in (-2, -1, 1, 2)]

    barrier = pltpu.get_barrier_semaphore()
    for s in range(1, GRP):
        pl.semaphore_signal(barrier, inc=1, device_id={"coil": lax.rem(j + s, GRP)}, device_id_type=MESH)
    for d, here in partners:
        @pl.when(here)
        def _():
            pl.semaphore_signal(barrier, inc=1, device_id={"frame": t + d}, device_id_type=MESH)

    loads[0].wait()
    xb[pl.ds(r0, RB), :] = image[...].astype(BF16)
    present = sum(here.astype(jnp.int32) for _, here in partners)
    pl.semaphore_wait(barrier, GRP - 1 + present)

    acopy = []
    for s in range(1, GRP):
        c = pltpu.make_async_remote_copy(
            src_ref=xb.at[pl.ds(r0, RB)],
            dst_ref=xb.at[pl.ds(r0, RB)],
            send_sem=asend.at[s],
            recv_sem=arecv.at[s],
            device_id={"coil": lax.rem(j + s, GRP)},
            device_id_type=MESH,
        )
        c.start()
        acopy.append(c)

    loads[1].wait()
    loads[2].wait()

    def columns(q):
        rq = pl.multiple_of(q * RB, RB)
        xv = xb[pl.ds(rq, RB), :].astype(F32)
        x_re, x_im = xv[:, :N], xv[:, N:]
        for c in range(NCO):
            sv = sens[c, pl.ds(rq, RB), :].astype(F32)
            s_re, s_im = sv[:, :N], sv[:, N:]
            ci[c * RB : (c + 1) * RB, :N] = (s_re * x_re - s_im * x_im).astype(BF16)
            ci[c * RB : (c + 1) * RB, N:] = (s_re * x_im + s_im * x_re).astype(BF16)
        for half in range(2):
            spec = dot(ci[...], ta[0, :, half * N : (half + 1) * N]).astype(BF16)
            for c in range(NCO):
                cols[c, pl.ds(half * ROWS + rq, RB), :] = spec[c * RB : (c + 1) * RB]

    columns(j)

    @pl.loop(1, GRP)
    def _(s):
        pltpu.make_async_remote_copy(
            src_ref=xb.at[pl.ds(r0, RB)],
            dst_ref=xb.at[pl.ds(pl.multiple_of(lax.rem(j - s + GRP, GRP) * RB, RB), RB)],
            send_sem=asend.at[s],
            recv_sem=arecv.at[s],
            device_id={"coil": lax.rem(j + s, GRP)},
            device_id_type=MESH,
        ).wait_recv()
        columns(lax.rem(j - s + GRP, GRP))

    loads[3].wait()
    loads[4].wait()
    loads[5].wait()

    for c in range(NCO):
        for half in range(2):
            est = dot(tb[0, half * ROWS : (half + 1) * ROWS, :], cols[c])
            k = ksp[c, :, half * N : (half + 1) * N].astype(F32)
            misfit[c, :, half * N : (half + 1) * N] = (est - k).astype(BF16)
    for c in range(NCO):
        for half in range(2):
            stacked[c, half * ROWS : (half + 1) * ROWS, :] = dot(
                misfit[c], ta[1, :, half * N : (half + 1) * N]
            ).astype(BF16)
    for c in range(NCO):
        m = mask[c : c + 1, :].astype(F32).astype(BF16)
        mm = jnp.concatenate([m, m], axis=1)
        b_re = dot(tb[1, :ROWS, :] * mm, stacked[c])
        b_im = dot(tb[1, ROWS:, :] * mm, stacked[c])
        s_re, s_im = sens[c, :, :N].astype(F32), sens[c, :, N:].astype(F32)
        g_re = s_re * b_re + s_im * b_im
        g_im = s_re * b_im - s_im * b_re
        acc[:, :N] = g_re if c == 0 else acc[:, :N] + g_re
        acc[:, N:] = g_im if c == 0 else acc[:, N:] + g_im

    gs[:ROWS, :] = pltpu.roll(acc[...], 3, axis=0).astype(BF16)
    gs[ROWS : ROWS + 16, :] = pltpu.roll(acc[ROWS - 16 :, :], 3, axis=0).astype(BF16)

    bcopy = []
    for s in range(1, GRP):
        to = lax.rem(j + s, GRP)
        c = pltpu.make_async_remote_copy(
            src_ref=gs.at[pl.ds(pl.multiple_of(to * RB, RB), HR)],
            dst_ref=grecv.at[s],
            send_sem=bsend.at[s],
            recv_sem=brecv.at[s],
            device_id={"coil": to},
            device_id_type=MESH,
        )
        c.start()
        bcopy.append(c)

    xr[:ROWS, :] = pltpu.roll(xb[...].astype(F32), 3, axis=0)
    xr[ROWS : ROWS + 16, :] = jnp.zeros((16, 2 * N), F32)
    x48[...] = xr[pl.ds(r0, HR), :]
    x48[3 : 3 + RB, :] = image[...]
    for c in loads[6:]:
        c.wait()
    total = x48[...] - gs[pl.ds(r0, HR), :].astype(F32)
    for c in bcopy:
        c.wait_recv()
    for s in range(1, GRP):
        total = total - grecv[s].astype(F32)
    row = r0 - 3 + lax.broadcasted_iota(jnp.int32, (HR, 2 * N), 0)
    total = jnp.where((row >= 0) & (row < ROWS), total, 0.0)
    x48[...] = total
    hb[2] = total.astype(BF16)

    for d, here in partners:
        def ccopy(d=d):
            return pltpu.make_async_remote_copy(
                src_ref=hb.at[2],
                dst_ref=hb.at[2 - d],
                send_sem=csend.at[d + 2],
                recv_sem=crecv.at[d + 2],
                device_id={"frame": t + d},
                device_id_type=MESH,
            )

        @pl.when(here)
        def _():
            ccopy().start()

        @pl.when(jnp.logical_not(here))
        def _():
            hb[2 + d] = jnp.zeros((HR, 2 * N), BF16)

    def planes(f):
        v = hb[f].astype(F32)
        parts = []
        for half in range(2):
            p = v[:, half * N : (half + 1) * N]
            parts += [shift_right(p), p, shift_left(p)]
        for i in range(HR // 8):
            kb[i, f * HR : (f + 1) * HR, :] = jnp.concatenate(
                [p[8 * i : 8 * i + 8] for p in parts], axis=0
            ).astype(BF16)

    planes(2)
    for d, here in partners:
        @pl.when(here)
        def _():
            pltpu.make_async_remote_copy(
                src_ref=hb.at[2],
                dst_ref=hb.at[2 + d],
                send_sem=csend.at[2 - d],
                recv_sem=crecv.at[2 - d],
                device_id={"frame": t + d},
                device_id_type=MESH,
            ).wait_recv()

        planes(2 + d)

    bias1 = b1[...]
    for f in range(3):
        for i in range(5):
            here_k = kb[i, f * HR : (f + 3) * HR, :]
            next_k = kb[i + 1, f * HR : (f + 3) * HR, :]
            top = dot(w1[:384, :], here_k)
            low = dot(w1[384:512, :], here_k) + dot(w1[512:, :], next_k)
            base = i * 512
            for q in range(6):
                h1[f, pl.ds(base + q * CH, CH), :] = jnp.maximum(top[q * CH : (q + 1) * CH] + bias1, 0.0).astype(BF16)
            for q in range(2):
                h1[f, pl.ds(base + (6 + q) * CH, CH), :] = jnp.maximum(low[q * CH : (q + 1) * CH] + bias1, 0.0).astype(BF16)

    @pl.when(j == 0)
    def _():
        h1[:, : 2 * CH, :] = jnp.zeros((3, 2 * CH, N), BF16)

    @pl.when(j == GRP - 1)
    def _():
        h1[:, 34 * CH :, :] = jnp.zeros((3, 6 * CH, N), BF16)

    @pl.when(t == 0)
    def _():
        h1[0] = jnp.zeros((40 * CH, N), BF16)

    @pl.when(t == frames - 1)
    def _():
        h1[2] = jnp.zeros((40 * CH, N), BF16)

    bias2 = b2[...]

    for r in range(34):
        base = r * CH
        taps = dot(w2[0], h1[0, base : base + 3 * CH, :])
        taps += dot(w2[1], h1[1, base : base + 3 * CH, :])
        taps += dot(w2[2], h1[2, base : base + 3 * CH, :])
        v = taps[CH : 2 * CH] + shift_right(taps[:CH]) + shift_left(taps[2 * CH :]) + bias2
        h2[base : base + CH, :] = jnp.maximum(v, 0.0).astype(BF16)

    @pl.when(j == 0)
    def _():
        h2[:CH, :] = jnp.zeros((CH, N), BF16)

    @pl.when(j == GRP - 1)
    def _():
        h2[33 * CH :, :] = jnp.zeros((CH, N), BF16)

    for i in range(RB // 8):
        base = i * 8 * CH
        taps = dot(w3[...], h2[base : base + 10 * CH, :])
        v = taps[48:96] + shift_right(taps[:48]) + shift_left(taps[96:])
        ri = i * 8
        for a in range(3):
            for half in range(2):
                o = (a * 2 + half) * 8
                psend[a, pl.ds(ri, 8), half * N : (half + 1) * N] = v[o : o + 8]

    ends = [(1, 0, t + 1 < frames), (-1, 2, t >= 1)]
    for n, (d, a, here) in enumerate(ends):
        @pl.when(here)
        def _():
            pltpu.make_async_remote_copy(
                src_ref=psend.at[a],
                dst_ref=precv.at[n],
                send_sem=dsend.at[n],
                recv_sem=drecv.at[n],
                device_id={"frame": t + d},
                device_id_type=MESH,
            ).start()

    out_ref[...] = x48[3 : 3 + RB, :] + psend[1]
    for n, (d, a, here) in enumerate(ends):
        @pl.when((t - d >= 0) & (t - d < frames))
        def _():
            pltpu.make_async_remote_copy(
                src_ref=psend.at[a],
                dst_ref=precv.at[n],
                send_sem=dsend.at[n],
                recv_sem=drecv.at[n],
                device_id={"frame": t - d},
                device_id_type=MESH,
            ).wait_recv()
            out_ref[...] += precv[n]

    for c in acopy + bcopy:
        c.wait_send()
    for d, here in partners:
        @pl.when(here)
        def _():
            pltpu.make_async_remote_copy(
                src_ref=hb.at[2],
                dst_ref=hb.at[2 - d],
                send_sem=csend.at[d + 2],
                recv_sem=crecv.at[d + 2],
                device_id={"frame": t + d},
                device_id_type=MESH,
            ).wait_send()
    for n, (d, a, here) in enumerate(ends):
        @pl.when(here)
        def _():
            pltpu.make_async_remote_copy(
                src_ref=psend.at[a],
                dst_ref=precv.at[n],
                send_sem=dsend.at[n],
                recv_sem=drecv.at[n],
                device_id={"frame": t + d},
                device_id_type=MESH,
            ).wait_send()


def spread(rows, width, first):
    out = np.zeros((3, rows, width), np.float32)
    for q in range(rows):
        for b in range(3):
            u = q + first + b
            if 0 <= u < width:
                out[b, q, u] = 1
    return out


def shards(frames, kspace, sens, mask, image, w_first, b_first, w_mid, b_mid, w_last):
    cols, back, rows, rback = dft_tables()
    ta = jnp.asarray(np.stack([cols, back]), BF16)
    tb = jnp.asarray(np.stack([rows, rback]), BF16)
    here = spread(8, 8, 0)
    ahead = spread(2, 8, -2)
    pick1 = jnp.asarray(np.concatenate([here, ahead], axis=1), BF16)
    w1 = jnp.einsum("abeoc,bqu->qoaceu", w_first, pick1).reshape(10 * CH, 3 * HR)
    w2 = jnp.transpose(w_mid, (0, 2, 3, 1, 4)).reshape(3, 3 * CH, 3 * CH)
    pick3 = jnp.asarray(spread(8, 10, 0), BF16)
    w3 = jnp.einsum("abeoi,bqu->eaoqui", w_last, pick3).reshape(144, 10 * CH)
    b1 = jnp.broadcast_to(b_first[:, None], (CH, N))
    b2 = jnp.broadcast_to(b_mid[:, None], (CH, N))
    args = (kspace[0], sens, mask[0], image[0], ta, tb, w1, w2, w3, b1, b2)
    order = args
    dma = pltpu.SemaphoreType.DMA
    out = pl.pallas_call(
        functools.partial(kernel, frames),
        out_shape=jax.ShapeDtypeStruct((RB, 2 * N), F32),
        in_specs=[pl.BlockSpec(memory_space=pl.ANY)] * len(args),
        out_specs=pl.BlockSpec(memory_space=pltpu.VMEM),
        scratch_shapes=[pltpu.VMEM(a.shape, a.dtype) for a in order]
        + [
            pltpu.VMEM((ROWS, 2 * N), BF16),
            pltpu.VMEM((NCO * RB, 2 * N), BF16),
            pltpu.VMEM((NCO, 2 * ROWS, N), BF16),
            pltpu.VMEM((NCO, ROWS, 2 * N), BF16),
            pltpu.VMEM((NCO, 2 * ROWS, N), BF16),
            pltpu.VMEM((ROWS, 2 * N), F32),
            pltpu.VMEM((ROWS + 16, 2 * N), BF16),
            pltpu.VMEM((GRP, HR, 2 * N), BF16),
            pltpu.VMEM((ROWS + 16, 2 * N), F32),
            pltpu.VMEM((HR, 2 * N), F32),
            pltpu.VMEM((5, HR, 2 * N), BF16),
            pltpu.VMEM((HR // 8, 5 * HR, N), BF16),
            pltpu.VMEM((3, 40 * CH, N), BF16),
            pltpu.VMEM((34 * CH, N), BF16),
            pltpu.VMEM((3, RB, 2 * N), F32),
            pltpu.VMEM((2, RB, 2 * N), F32),
            dma((len(args),)), dma((GRP,)), dma((GRP,)), dma((GRP,)), dma((GRP,)),
            dma((5,)), dma((5,)), dma((2,)), dma((2,)),
        ],
        compiler_params=pltpu.CompilerParams(
            collective_id=0, has_side_effects=True, vmem_limit_bytes=56 * 1024 * 1024
        ),
    )(*args)
    return out[None]


def solution(mesh):
    in_specs = (
        P("frame", "coil", None, None),
        P("coil", None, None),
        P("frame", "coil", None),
        P("frame", "coil", None),
        P(),
        P(),
        P(),
        P(),
        P(),
    )
    out_specs = P("frame", "coil", None)
    body = functools.partial(shards, mesh.shape["frame"])
    return jax.shard_map(body, mesh=mesh, in_specs=in_specs, out_specs=out_specs, check_vma=False)
```

```python
import functools

import jax
import jax.numpy as jnp
import numpy as np
from jax import lax
from jax.experimental import pallas as pl
from jax.experimental.pallas import tpu as pltpu
from jax.sharding import PartitionSpec as P

F32 = jnp.float32
BF16 = jnp.bfloat16
MESH = pl.DeviceIdType.MESH

ROWS = 256
N = 256
RB = 32
HR = 48
NCO = 8
CH = 64
GRP = 8


def dft_tables():
    idx = np.arange(N)
    ang = (idx[:, None] * idx[None, :] % N) * (2.0 * np.pi / N)
    fr = (np.cos(ang) / np.sqrt(N)).astype(np.float32)
    fi = (-np.sin(ang) / np.sqrt(N)).astype(np.float32)
    return np.stack([np.block([[fr, fi], [-fi, fr]]), np.block([[fr, -fi], [fi, fr]])])


def shift_right(v):
    lane = lax.broadcasted_iota(jnp.int32, v.shape, 1)
    return jnp.where(lane == 0, 0.0, pltpu.roll(v, 1, axis=1))


def shift_left(v):
    lane = lax.broadcasted_iota(jnp.int32, v.shape, 1)
    return jnp.where(lane == N - 1, 0.0, pltpu.roll(v, N - 1, axis=1))


def dot(a, b):
    return jnp.dot(a, b, preferred_element_type=F32)


def iota2(shape):
    return lax.broadcasted_iota(jnp.int32, shape, 0), lax.broadcasted_iota(jnp.int32, shape, 1)


def conv_weights(pick, wf, wm, wl, bf, bm, w54, w1, w2, w3):
    w54[...] = jnp.zeros((64, CH), F32)
    for k in range(27):
        w54[2 * k : 2 * k + 2, :] = wf[k].astype(F32)
    source = w54[...].astype(BF16)
    row, col = iota2((640, CH))
    tile = ((row & (CH - 1)) == col).astype(F32).astype(BF16)
    row, col = iota2((640, 144))
    base = jnp.where(row >= 512, (row >> 6) - 10, row >> 6)
    total = jnp.zeros((640, 144), F32)
    for b in range(3):
        z = dot(pick[b], source).astype(BF16)
        part = lax.dot_general(tile, z, (((1,), (1,)), ((), ())), preferred_element_type=F32)
        total = jnp.where((col & 7) == base + b, part, total)
    w1[...] = total.astype(BF16)
    for k in range(27):
        w54[2 * k : 2 * k + 2, :] = wl[k].astype(F32)
    source = w54[...].astype(BF16)
    row, col = iota2((CH, 640))
    tile = (row == (col & (CH - 1))).astype(F32).astype(BF16)
    row, col = iota2((144, 640))
    total = jnp.zeros((144, 640), F32)
    for b in range(3):
        z = dot(pick[3 + b], source).astype(BF16)
        total = jnp.where((col >> 6) == (row & 7) + b, dot(z, tile), total)
    w3[...] = total.astype(BF16)
    row, col = iota2((CH, 3 * CH))
    places = [(col == row + b * CH).astype(F32).astype(BF16) for b in range(3)]
    for a in range(3):
        for e in range(3):
            w2[a, e * CH : (e + 1) * CH, :] = sum(
                dot(wm[(a * 3 + b) * 3 + e], places[b]) for b in range(3)
            ).astype(BF16)
    return [jnp.broadcast_to(v[...], (N, CH)).T for v in (bf, bm)]


def kernel(
    frames,
    kspace_hbm, sens_hbm, mask_hbm, image_hbm, table_hbm, pick_hbm, wf_hbm, wm_hbm, wl_hbm, bf_hbm, bm_hbm,
    out_ref,
    ksp, sens, mask, image, table, pick, wf, wm, wl, bf, bm,
    w54, w1, w2, w3,
    xb, ci, cols, misfit, stacked, acc, gs, grecv, xr, x48, hb, kb, h1, h2, psend, precv,
    lsem, asend, arecv, bsend, brecv, csend, crecv, dsend, drecv,
):
    t = lax.axis_index("frame")
    j = lax.axis_index("coil")
    r0 = pl.multiple_of(j * RB, RB)

    loads = [
        pltpu.make_async_copy(src, dst, lsem.at[i])
        for i, (src, dst) in enumerate(
            [
                (image_hbm, image), (pick_hbm, pick), (wf_hbm, wf), (wm_hbm, wm), (wl_hbm, wl), (bf_hbm, bf),
                (bm_hbm, bm), (sens_hbm, sens), (table_hbm, table), (kspace_hbm, ksp), (mask_hbm, mask),
            ]
        )
    ]
    for c in loads:
        c.start()

    partners = [(d, (t + d >= 0) & (t + d < frames)) for d in (-2, -1, 1, 2)]

    barrier = pltpu.get_barrier_semaphore()
    for s in range(1, GRP):
        pl.semaphore_signal(barrier, inc=1, device_id={"coil": lax.rem(j + s, GRP)}, device_id_type=MESH)
    for d, here in partners:
        @pl.when(here)
        def _():
            pl.semaphore_signal(barrier, inc=1, device_id={"frame": t + d}, device_id_type=MESH)

    loads[0].wait()
    xb[pl.ds(r0, RB), :] = image[...].astype(BF16)
    for c in loads[1:7]:
        c.wait()
    bias1, bias2 = conv_weights(pick, wf, wm, wl, bf, bm, w54, w1, w2, w3)
    present = sum(here.astype(jnp.int32) for _, here in partners)
    pl.semaphore_wait(barrier, GRP - 1 + present)

    acopy = []
    for s in range(1, GRP):
        c = pltpu.make_async_remote_copy(
            src_ref=xb.at[pl.ds(r0, RB)],
            dst_ref=xb.at[pl.ds(r0, RB)],
            send_sem=asend.at[s],
            recv_sem=arecv.at[s],
            device_id={"coil": lax.rem(j + s, GRP)},
            device_id_type=MESH,
        )
        c.start()
        acopy.append(c)

    loads[7].wait()
    loads[8].wait()

    def columns(q):
        rq = pl.multiple_of(q * RB, RB)
        xv = xb[pl.ds(rq, RB), :].astype(F32)
        x_re, x_im = xv[:, :N], xv[:, N:]
        for c in range(NCO):
            sv = sens[c, pl.ds(rq, RB), :].astype(F32)
            s_re, s_im = sv[:, :N], sv[:, N:]
            ci[c * RB : (c + 1) * RB, :N] = (s_re * x_re - s_im * x_im).astype(BF16)
            ci[c * RB : (c + 1) * RB, N:] = (s_re * x_im + s_im * x_re).astype(BF16)
        for half in range(2):
            spec = dot(ci[...], table[0, :, half * N : (half + 1) * N]).astype(BF16)
            for c in range(NCO):
                cols[c, pl.ds(half * ROWS + rq, RB), :] = spec[c * RB : (c + 1) * RB]

    columns(j)

    @pl.loop(1, GRP)
    def _(s):
        pltpu.make_async_remote_copy(
            src_ref=xb.at[pl.ds(r0, RB)],
            dst_ref=xb.at[pl.ds(pl.multiple_of(lax.rem(j - s + GRP, GRP) * RB, RB), RB)],
            send_sem=asend.at[s],
            recv_sem=arecv.at[s],
            device_id={"coil": lax.rem(j + s, GRP)},
            device_id_type=MESH,
        ).wait_recv()
        columns(lax.rem(j - s + GRP, GRP))

    loads[9].wait()
    loads[10].wait()

    for c in range(NCO):
        for half in range(2):
            est = dot(table[1, half * ROWS : (half + 1) * ROWS, :], cols[c])
            k = ksp[c, :, half * N : (half + 1) * N].astype(F32)
            misfit[c, :, half * N : (half + 1) * N] = (est - k).astype(BF16)
    for c in range(NCO):
        for half in range(2):
            stacked[c, half * ROWS : (half + 1) * ROWS, :] = dot(
                misfit[c], table[1, :, half * N : (half + 1) * N]
            ).astype(BF16)
    for c in range(NCO):
        m = mask[c : c + 1, :].astype(F32).astype(BF16)
        mm = jnp.concatenate([m, m], axis=1)
        b_re = dot(table[0, :ROWS, :] * mm, stacked[c])
        b_im = dot(table[0, ROWS:, :] * mm, stacked[c])
        s_re, s_im = sens[c, :, :N].astype(F32), sens[c, :, N:].astype(F32)
        g_re = s_re * b_re + s_im * b_im
        g_im = s_re * b_im - s_im * b_re
        acc[:, :N] = g_re if c == 0 else acc[:, :N] + g_re
        acc[:, N:] = g_im if c == 0 else acc[:, N:] + g_im

    gs[:ROWS, :] = pltpu.roll(acc[...], 3, axis=0).astype(BF16)
    gs[ROWS : ROWS + 16, :] = pltpu.roll(acc[ROWS - 16 :, :], 3, axis=0).astype(BF16)

    bcopy = []
    for s in range(1, GRP):
        to = lax.rem(j + s, GRP)
        c = pltpu.make_async_remote_copy(
            src_ref=gs.at[pl.ds(pl.multiple_of(to * RB, RB), HR)],
            dst_ref=grecv.at[s],
            send_sem=bsend.at[s],
            recv_sem=brecv.at[s],
            device_id={"coil": to},
            device_id_type=MESH,
        )
        c.start()
        bcopy.append(c)

    xr[:ROWS, :] = pltpu.roll(xb[...].astype(F32), 3, axis=0)
    xr[ROWS : ROWS + 16, :] = jnp.zeros((16, 2 * N), F32)
    x48[...] = xr[pl.ds(r0, HR), :]
    x48[3 : 3 + RB, :] = image[...]
    total = x48[...] - gs[pl.ds(r0, HR), :].astype(F32)
    for c in bcopy:
        c.wait_recv()
    for s in range(1, GRP):
        total = total - grecv[s].astype(F32)
    row = r0 - 3 + lax.broadcasted_iota(jnp.int32, (HR, 2 * N), 0)
    total = jnp.where((row >= 0) & (row < ROWS), total, 0.0)
    x48[...] = total
    hb[2] = total.astype(BF16)

    for d, here in partners:
        def ccopy(d=d):
            return pltpu.make_async_remote_copy(
                src_ref=hb.at[2],
                dst_ref=hb.at[2 - d],
                send_sem=csend.at[d + 2],
                recv_sem=crecv.at[d + 2],
                device_id={"frame": t + d},
                device_id_type=MESH,
            )

        @pl.when(here)
        def _():
            ccopy().start()

        @pl.when(jnp.logical_not(here))
        def _():
            hb[2 + d] = jnp.zeros((HR, 2 * N), BF16)

    def planes(f):
        v = hb[f].astype(F32)
        parts = []
        for half in range(2):
            p = v[:, half * N : (half + 1) * N]
            parts += [shift_right(p), p, shift_left(p)]
        for i in range(HR // 8):
            kb[i, f * HR : (f + 1) * HR, :] = jnp.concatenate(
                [p[8 * i : 8 * i + 8] for p in parts], axis=0
            ).astype(BF16)

    planes(2)
    for d, here in partners:
        @pl.when(here)
        def _():
            pltpu.make_async_remote_copy(
                src_ref=hb.at[2],
                dst_ref=hb.at[2 + d],
                send_sem=csend.at[2 - d],
                recv_sem=crecv.at[2 - d],
                device_id={"frame": t + d},
                device_id_type=MESH,
            ).wait_recv()

        planes(2 + d)

    for f in range(3):
        for i in range(5):
            here_k = kb[i, f * HR : (f + 3) * HR, :]
            next_k = kb[i + 1, f * HR : (f + 3) * HR, :]
            top = dot(w1[:384, :], here_k)
            low = dot(w1[384:512, :], here_k) + dot(w1[512:, :], next_k)
            base = i * 512
            for q in range(6):
                h1[f, pl.ds(base + q * CH, CH), :] = jnp.maximum(top[q * CH : (q + 1) * CH] + bias1, 0.0).astype(BF16)
            for q in range(2):
                h1[f, pl.ds(base + (6 + q) * CH, CH), :] = jnp.maximum(low[q * CH : (q + 1) * CH] + bias1, 0.0).astype(BF16)

    @pl.when(j == 0)
    def _():
        h1[:, : 2 * CH, :] = jnp.zeros((3, 2 * CH, N), BF16)

    @pl.when(j == GRP - 1)
    def _():
        h1[:, 34 * CH :, :] = jnp.zeros((3, 6 * CH, N), BF16)

    @pl.when(t == 0)
    def _():
        h1[0] = jnp.zeros((40 * CH, N), BF16)

    @pl.when(t == frames - 1)
    def _():
        h1[2] = jnp.zeros((40 * CH, N), BF16)

    for r in range(34):
        base = r * CH
        taps = dot(w2[0], h1[0, base : base + 3 * CH, :])
        taps += dot(w2[1], h1[1, base : base + 3 * CH, :])
        taps += dot(w2[2], h1[2, base : base + 3 * CH, :])
        v = taps[CH : 2 * CH] + shift_right(taps[:CH]) + shift_left(taps[2 * CH :]) + bias2
        h2[base : base + CH, :] = jnp.maximum(v, 0.0).astype(BF16)

    @pl.when(j == 0)
    def _():
        h2[:CH, :] = jnp.zeros((CH, N), BF16)

    @pl.when(j == GRP - 1)
    def _():
        h2[33 * CH :, :] = jnp.zeros((CH, N), BF16)

    for i in range(RB // 8):
        base = i * 8 * CH
        taps = dot(w3[...], h2[base : base + 10 * CH, :])
        v = taps[48:96] + shift_right(taps[:48]) + shift_left(taps[96:])
        ri = i * 8
        for a in range(3):
            for half in range(2):
                o = (a * 2 + half) * 8
                psend[a, pl.ds(ri, 8), half * N : (half + 1) * N] = v[o : o + 8]

    ends = [(1, 0, t + 1 < frames), (-1, 2, t >= 1)]
    for n, (d, a, here) in enumerate(ends):
        @pl.when(here)
        def _():
            pltpu.make_async_remote_copy(
                src_ref=psend.at[a],
                dst_ref=precv.at[n],
                send_sem=dsend.at[n],
                recv_sem=drecv.at[n],
                device_id={"frame": t + d},
                device_id_type=MESH,
            ).start()

    out_ref[...] = x48[3 : 3 + RB, :] + psend[1]
    for n, (d, a, here) in enumerate(ends):
        @pl.when((t - d >= 0) & (t - d < frames))
        def _():
            pltpu.make_async_remote_copy(
                src_ref=psend.at[a],
                dst_ref=precv.at[n],
                send_sem=dsend.at[n],
                recv_sem=drecv.at[n],
                device_id={"frame": t - d},
                device_id_type=MESH,
            ).wait_recv()
            out_ref[...] += precv[n]

    for c in acopy + bcopy:
        c.wait_send()
    for d, here in partners:
        @pl.when(here)
        def _():
            pltpu.make_async_remote_copy(
                src_ref=hb.at[2],
                dst_ref=hb.at[2 - d],
                send_sem=csend.at[d + 2],
                recv_sem=crecv.at[d + 2],
                device_id={"frame": t + d},
                device_id_type=MESH,
            ).wait_send()
    for n, (d, a, here) in enumerate(ends):
        @pl.when(here)
        def _():
            pltpu.make_async_remote_copy(
                src_ref=psend.at[a],
                dst_ref=precv.at[n],
                send_sem=dsend.at[n],
                recv_sem=drecv.at[n],
                device_id={"frame": t + d},
                device_id_type=MESH,
            ).wait_send()


def picks():
    out = np.zeros((6, 144, 64), np.float32)
    for b in range(3):
        for k in range(18):
            a, ch, e = k // 6, k // 3 % 2, k % 3
            out[b, 8 * k : 8 * k + 8, ((a * 3 + b) * 3 + e) * 2 + ch] = 1
            e, a, ch = k // 6, k // 2 % 3, k % 2
            out[3 + b, 8 * k : 8 * k + 8, ((a * 3 + b) * 3 + e) * 2 + ch] = 1
    return out


def shards(frames, kspace, sens, mask, image, w_first, b_first, w_mid, b_mid, w_last):
    args = (
        kspace[0], sens, mask[0], image[0], jnp.asarray(dft_tables(), BF16), jnp.asarray(picks(), BF16),
        jnp.swapaxes(w_first, 3, 4).reshape(27, 2, CH), w_mid.reshape(27, CH, CH), w_last.reshape(27, 2, CH),
        b_first[None], b_mid[None],
    )
    dma = pltpu.SemaphoreType.DMA
    out = pl.pallas_call(
        functools.partial(kernel, frames),
        out_shape=jax.ShapeDtypeStruct((RB, 2 * N), F32),
        in_specs=[pl.BlockSpec(memory_space=pl.ANY)] * len(args),
        out_specs=pl.BlockSpec(memory_space=pltpu.VMEM),
        scratch_shapes=[pltpu.VMEM(a.shape, a.dtype) for a in args]
        + [
            pltpu.VMEM((64, CH), F32),
            pltpu.VMEM((640, 144), BF16),
            pltpu.VMEM((3, 3 * CH, 3 * CH), BF16),
            pltpu.VMEM((144, 640), BF16),
            pltpu.VMEM((ROWS, 2 * N), BF16),
            pltpu.VMEM((NCO * RB, 2 * N), BF16),
            pltpu.VMEM((NCO, 2 * ROWS, N), BF16),
            pltpu.VMEM((NCO, ROWS, 2 * N), BF16),
            pltpu.VMEM((NCO, 2 * ROWS, N), BF16),
            pltpu.VMEM((ROWS, 2 * N), F32),
            pltpu.VMEM((ROWS + 16, 2 * N), BF16),
            pltpu.VMEM((GRP, HR, 2 * N), BF16),
            pltpu.VMEM((ROWS + 16, 2 * N), F32),
            pltpu.VMEM((HR, 2 * N), F32),
            pltpu.VMEM((5, HR, 2 * N), BF16),
            pltpu.VMEM((HR // 8, 5 * HR, N), BF16),
            pltpu.VMEM((3, 40 * CH, N), BF16),
            pltpu.VMEM((34 * CH, N), BF16),
            pltpu.VMEM((3, RB, 2 * N), F32),
            pltpu.VMEM((2, RB, 2 * N), F32),
            dma((len(args),)), dma((GRP,)), dma((GRP,)), dma((GRP,)), dma((GRP,)),
            dma((5,)), dma((5,)), dma((2,)), dma((2,)),
        ],
        compiler_params=pltpu.CompilerParams(
            collective_id=0, has_side_effects=True, vmem_limit_bytes=56 * 1024 * 1024
        ),
    )(*args)
    return out[None]


def solution(mesh):
    in_specs = (
        P("frame", "coil", None, None),
        P("coil", None, None),
        P("frame", "coil", None),
        P("frame", "coil", None),
        P(),
        P(),
        P(),
        P(),
        P(),
    )
    out_specs = P("frame", "coil", None)
    body = functools.partial(shards, mesh.shape["frame"])
    return jax.shard_map(body, mesh=mesh, in_specs=in_specs, out_specs=out_specs, check_vma=False)
```

```python
import functools

import jax
import jax.numpy as jnp
import numpy as np
from jax import lax
from jax.experimental import pallas as pl
from jax.experimental.pallas import tpu as pltpu
from jax.sharding import PartitionSpec as P

F32 = jnp.float32
BF16 = jnp.bfloat16
MESH = pl.DeviceIdType.MESH

ROWS = 256
N = 256
RB = 32
HR = 40
KF = 48
NCO = 8
CH = 64
GRP = 8


def dft_tables():
    idx = np.arange(N)
    ang = (idx[:, None] * idx[None, :] % N) * (2.0 * np.pi / N)
    fr = (np.cos(ang) / np.sqrt(N)).astype(np.float32)
    fi = (-np.sin(ang) / np.sqrt(N)).astype(np.float32)
    return np.stack([np.block([[fr, fi], [-fi, fr]]), np.block([[fr, -fi], [fi, fr]])])


def shift_right(v):
    lane = lax.broadcasted_iota(jnp.int32, v.shape, 1)
    return jnp.where(lane == 0, 0.0, pltpu.roll(v, 1, axis=1))


def shift_left(v):
    lane = lax.broadcasted_iota(jnp.int32, v.shape, 1)
    return jnp.where(lane == N - 1, 0.0, pltpu.roll(v, N - 1, axis=1))


def dot(a, b):
    return jnp.dot(a, b, preferred_element_type=F32)


def iota2(shape):
    return lax.broadcasted_iota(jnp.int32, shape, 0), lax.broadcasted_iota(jnp.int32, shape, 1)


def conv_weights(pick, wf, wm, wl, bf, bm, w54, w1, w2, w3):
    w54[...] = jnp.zeros((64, CH), F32)
    for k in range(27):
        w54[2 * k : 2 * k + 2, :] = wf[k].astype(F32)
    source = w54[...].astype(BF16)
    row, col = iota2((640, CH))
    tile = ((row & (CH - 1)) == col).astype(F32).astype(BF16)
    row, col = iota2((640, 144))
    base = jnp.where(row >= 512, (row >> 6) - 10, row >> 6)
    total = jnp.zeros((640, 144), F32)
    for b in range(3):
        z = dot(pick[b], source).astype(BF16)
        part = lax.dot_general(tile, z, (((1,), (1,)), ((), ())), preferred_element_type=F32)
        total = jnp.where((col & 7) == base + b, part, total)
    w1[...] = total.astype(BF16)
    for k in range(27):
        w54[2 * k : 2 * k + 2, :] = wl[k].astype(F32)
    source = w54[...].astype(BF16)
    row, col = iota2((CH, 640))
    tile = (row == (col & (CH - 1))).astype(F32).astype(BF16)
    row, col = iota2((144, 640))
    total = jnp.zeros((144, 640), F32)
    for b in range(3):
        z = dot(pick[3 + b], source).astype(BF16)
        total = jnp.where((col >> 6) == (row & 7) + b, dot(z, tile), total)
    w3[...] = total.astype(BF16)
    row, col = iota2((CH, 3 * CH))
    places = [(col == row + b * CH).astype(F32).astype(BF16) for b in range(3)]
    for a in range(3):
        for e in range(3):
            w2[a, e * CH : (e + 1) * CH, :] = sum(
                dot(wm[(a * 3 + b) * 3 + e], places[b]) for b in range(3)
            ).astype(BF16)
    return [jnp.broadcast_to(v[...], (N, CH)).T for v in (bf, bm)]


def kernel(
    frames,
    kspace_hbm, sens_hbm, mask_hbm, image_hbm, table_hbm, pick_hbm, wf_hbm, wm_hbm, wl_hbm, bf_hbm, bm_hbm,
    out_ref,
    ksp, sens, mask, image, table, pick, wf, wm, wl, bf, bm,
    w54, w1, w2, w3,
    xb, ci, cols, misfit, stacked, acc, gs, grecv, xr, xh, hb, kb, h1, h2, psend, precv,
    lsem, asend, arecv, bsend, brecv, csend, crecv, dsend, drecv,
):
    t = lax.axis_index("frame")
    j = lax.axis_index("coil")
    r0 = pl.multiple_of(j * RB, RB)

    loads = [
        pltpu.make_async_copy(src, dst, lsem.at[i])
        for i, (src, dst) in enumerate(
            [
                (image_hbm, image), (pick_hbm, pick), (wf_hbm, wf), (wm_hbm, wm), (wl_hbm, wl), (bf_hbm, bf),
                (bm_hbm, bm), (sens_hbm, sens), (table_hbm, table), (kspace_hbm, ksp), (mask_hbm, mask),
            ]
        )
    ]
    for c in loads:
        c.start()

    partners = [(d, (t + d >= 0) & (t + d < frames)) for d in (-2, 2, -1, 1)]

    barrier = pltpu.get_barrier_semaphore()
    for s in range(1, GRP):
        pl.semaphore_signal(barrier, inc=1, device_id={"coil": lax.rem(j + s, GRP)}, device_id_type=MESH)
    for d, here in partners:
        @pl.when(here)
        def _():
            pl.semaphore_signal(barrier, inc=1, device_id={"frame": t + d}, device_id_type=MESH)

    loads[0].wait()
    xb[pl.ds(r0, RB), :] = image[...].astype(BF16)
    for c in loads[1:7]:
        c.wait()
    bias1, bias2 = conv_weights(pick, wf, wm, wl, bf, bm, w54, w1, w2, w3)
    present = sum(here.astype(jnp.int32) for _, here in partners)
    pl.semaphore_wait(barrier, GRP - 1 + present)

    acopy = []
    for s in range(1, GRP):
        c = pltpu.make_async_remote_copy(
            src_ref=xb.at[pl.ds(r0, RB)],
            dst_ref=xb.at[pl.ds(r0, RB)],
            send_sem=asend.at[s],
            recv_sem=arecv.at[s],
            device_id={"coil": lax.rem(j + s, GRP)},
            device_id_type=MESH,
        )
        c.start()
        acopy.append(c)

    loads[7].wait()
    loads[8].wait()

    def columns(q):
        rq = pl.multiple_of(q * RB, RB)
        xv = xb[pl.ds(rq, RB), :].astype(F32)
        x_re, x_im = xv[:, :N], xv[:, N:]
        for c in range(NCO):
            sv = sens[c, pl.ds(rq, RB), :].astype(F32)
            s_re, s_im = sv[:, :N], sv[:, N:]
            ci[c * RB : (c + 1) * RB, :N] = (s_re * x_re - s_im * x_im).astype(BF16)
            ci[c * RB : (c + 1) * RB, N:] = (s_re * x_im + s_im * x_re).astype(BF16)
        for half in range(2):
            spec = dot(ci[...], table[0, :, half * N : (half + 1) * N]).astype(BF16)
            for c in range(NCO):
                cols[c, pl.ds(half * ROWS + rq, RB), :] = spec[c * RB : (c + 1) * RB]

    columns(j)

    @pl.loop(1, GRP)
    def _(s):
        pltpu.make_async_remote_copy(
            src_ref=xb.at[pl.ds(r0, RB)],
            dst_ref=xb.at[pl.ds(pl.multiple_of(lax.rem(j - s + GRP, GRP) * RB, RB), RB)],
            send_sem=asend.at[s],
            recv_sem=arecv.at[s],
            device_id={"coil": lax.rem(j + s, GRP)},
            device_id_type=MESH,
        ).wait_recv()
        columns(lax.rem(j - s + GRP, GRP))

    loads[9].wait()
    loads[10].wait()

    for c in range(NCO):
        for half in range(2):
            est = dot(table[1, half * ROWS : (half + 1) * ROWS, :], cols[c])
            k = ksp[c, :, half * N : (half + 1) * N].astype(F32)
            misfit[c, :, half * N : (half + 1) * N] = (est - k).astype(BF16)
    for c in range(NCO):
        for half in range(2):
            stacked[c, half * ROWS : (half + 1) * ROWS, :] = dot(
                misfit[c], table[1, :, half * N : (half + 1) * N]
            ).astype(BF16)
    for c in range(NCO):
        m = mask[c : c + 1, :].astype(F32).astype(BF16)
        mm = jnp.concatenate([m, m], axis=1)
        b_re = dot(table[0, :ROWS, :] * mm, stacked[c])
        b_im = dot(table[0, ROWS:, :] * mm, stacked[c])
        s_re, s_im = sens[c, :, :N].astype(F32), sens[c, :, N:].astype(F32)
        g_re = s_re * b_re + s_im * b_im
        g_im = s_re * b_im - s_im * b_re
        acc[:, :N] = g_re if c == 0 else acc[:, :N] + g_re
        acc[:, N:] = g_im if c == 0 else acc[:, N:] + g_im

    xr[:ROWS, :] = pltpu.roll(acc[...], 3, axis=0)
    xr[ROWS:, :] = pltpu.roll(acc[ROWS - 16 :, :], 3, axis=0)
    for q in range(GRP):
        rows = slice(q * RB, q * RB + HR)
        gs[q] = jnp.concatenate([xr[rows, :N], xr[rows, N:]], axis=0).astype(BF16)

    bcopy = []
    for s in range(1, GRP):
        to = lax.rem(j + s, GRP)
        c = pltpu.make_async_remote_copy(
            src_ref=gs.at[to],
            dst_ref=grecv.at[s],
            send_sem=bsend.at[s],
            recv_sem=brecv.at[s],
            device_id={"coil": to},
            device_id_type=MESH,
        )
        c.start()
        bcopy.append(c)

    xr[:ROWS, :] = pltpu.roll(xb[...].astype(F32), 3, axis=0)
    xr[ROWS:, :] = jnp.zeros((16, 2 * N), F32)
    for half in range(2):
        cut = slice(half * N, (half + 1) * N)
        xh[half * HR : (half + 1) * HR, :] = xr[pl.ds(r0, HR), cut]
        xh[half * HR + 3 : half * HR + 3 + RB, :] = image[:, cut]
    total = xh[...] - gs[j].astype(F32)
    for c in bcopy:
        c.wait_recv()
    for s in range(1, GRP):
        total = total - grecv[s].astype(F32)
    line = lax.broadcasted_iota(jnp.int32, (2 * HR, N), 0)
    row = r0 - 3 + jnp.where(line >= HR, line - HR, line)
    total = jnp.where((row >= 0) & (row < ROWS), total, 0.0)
    xh[...] = total
    hb[2] = total.astype(BF16)

    for d, here in partners:
        def ccopy(d=d):
            return pltpu.make_async_remote_copy(
                src_ref=hb.at[2],
                dst_ref=hb.at[2 - d],
                send_sem=csend.at[d + 2],
                recv_sem=crecv.at[d + 2],
                device_id={"frame": t + d},
                device_id_type=MESH,
            )

        @pl.when(here)
        def _():
            ccopy().start()

        @pl.when(jnp.logical_not(here))
        def _():
            hb[2 + d] = jnp.zeros((2 * HR, N), BF16)

    def planes(f):
        v = hb[f].astype(F32)
        parts = []
        for half in range(2):
            p = v[half * HR : (half + 1) * HR]
            parts += [shift_right(p), p, shift_left(p)]
        for i in range(HR // 8):
            kb[i, f * KF : (f + 1) * KF, :] = jnp.concatenate(
                [p[8 * i : 8 * i + 8] for p in parts], axis=0
            ).astype(BF16)

    def arrived(d):
        @pl.when((t + d >= 0) & (t + d < frames))
        def _():
            pltpu.make_async_remote_copy(
                src_ref=hb.at[2],
                dst_ref=hb.at[2 + d],
                send_sem=csend.at[2 - d],
                recv_sem=crecv.at[2 - d],
                device_id={"frame": t + d},
                device_id_type=MESH,
            ).wait_recv()

        planes(2 + d)

    def first(f):
        def put(q, v):
            h1[f, q * CH : (q + 1) * CH, :] = jnp.maximum(v + bias1, 0.0).astype(BF16)

        for i in range(5):
            here_k = kb[i, f * KF : (f + 3) * KF, :]
            if i == 4:
                top = dot(w1[: 4 * CH, :], here_k)
                for q in range(4):
                    put(32 + q, top[q * CH : (q + 1) * CH])
                continue
            next_k = kb[i + 1, f * KF : (f + 3) * KF, :]
            top = dot(w1[: 6 * CH, :], here_k)
            low = dot(w1[6 * CH : 8 * CH, :], here_k) + dot(w1[8 * CH :, :], next_k)
            for q in range(6):
                put(8 * i + q, top[q * CH : (q + 1) * CH])
            for q in range(2):
                put(8 * i + 6 + q, low[q * CH : (q + 1) * CH])

    planes(2)
    arrived(-1)
    arrived(1)
    first(1)
    arrived(-2)
    first(0)
    arrived(2)
    first(2)

    @pl.when(j == 0)
    def _():
        h1[:, : 2 * CH, :] = jnp.zeros((3, 2 * CH, N), BF16)

    @pl.when(j == GRP - 1)
    def _():
        h1[:, 34 * CH :, :] = jnp.zeros((3, 2 * CH, N), BF16)

    @pl.when(t == 0)
    def _():
        h1[0] = jnp.zeros((36 * CH, N), BF16)

    @pl.when(t == frames - 1)
    def _():
        h1[2] = jnp.zeros((36 * CH, N), BF16)

    for r in range(34):
        base = r * CH
        taps = dot(w2[0], h1[0, base : base + 3 * CH, :])
        taps += dot(w2[1], h1[1, base : base + 3 * CH, :])
        taps += dot(w2[2], h1[2, base : base + 3 * CH, :])
        v = taps[CH : 2 * CH] + shift_right(taps[:CH]) + shift_left(taps[2 * CH :]) + bias2
        h2[base : base + CH, :] = jnp.maximum(v, 0.0).astype(BF16)

    @pl.when(j == 0)
    def _():
        h2[:CH, :] = jnp.zeros((CH, N), BF16)

    @pl.when(j == GRP - 1)
    def _():
        h2[33 * CH :, :] = jnp.zeros((CH, N), BF16)

    blocks = []
    for i in range(RB // 8):
        base = i * 8 * CH
        taps = dot(w3[...], h2[base : base + 10 * CH, :])
        blocks.append(taps[48:96] + shift_right(taps[:48]) + shift_left(taps[96:]))
    for a in (0, 2, 1):
        for half in range(2):
            o = (a * 2 + half) * 8
            v = jnp.concatenate([b[o : o + 8] for b in blocks], axis=0)
            cut = slice(half * N, (half + 1) * N)
            if a == 1:
                xh[half * HR + 3 : half * HR + 3 + RB, :] += v
            else:
                psend[a // 2, :, cut] = v.astype(BF16)

    ends = [(1, 0, t + 1 < frames), (-1, 1, t >= 1)]
    for n, (d, a, here) in enumerate(ends):
        @pl.when(here)
        def _():
            pltpu.make_async_remote_copy(
                src_ref=psend.at[a],
                dst_ref=precv.at[n],
                send_sem=dsend.at[n],
                recv_sem=drecv.at[n],
                device_id={"frame": t + d},
                device_id_type=MESH,
            ).start()

    for half in range(2):
        out_ref[:, half * N : (half + 1) * N] = xh[half * HR + 3 : half * HR + 3 + RB, :]
    for n, (d, a, here) in enumerate(ends):
        @pl.when((t - d >= 0) & (t - d < frames))
        def _():
            pltpu.make_async_remote_copy(
                src_ref=psend.at[a],
                dst_ref=precv.at[n],
                send_sem=dsend.at[n],
                recv_sem=drecv.at[n],
                device_id={"frame": t - d},
                device_id_type=MESH,
            ).wait_recv()
            out_ref[...] += precv[n].astype(F32)

    for c in acopy + bcopy:
        c.wait_send()
    for d, here in partners:
        @pl.when(here)
        def _():
            pltpu.make_async_remote_copy(
                src_ref=hb.at[2],
                dst_ref=hb.at[2 - d],
                send_sem=csend.at[d + 2],
                recv_sem=crecv.at[d + 2],
                device_id={"frame": t + d},
                device_id_type=MESH,
            ).wait_send()
    for n, (d, a, here) in enumerate(ends):
        @pl.when(here)
        def _():
            pltpu.make_async_remote_copy(
                src_ref=psend.at[a],
                dst_ref=precv.at[n],
                send_sem=dsend.at[n],
                recv_sem=drecv.at[n],
                device_id={"frame": t + d},
                device_id_type=MESH,
            ).wait_send()


def picks():
    out = np.zeros((6, 144, 64), np.float32)
    for b in range(3):
        for k in range(18):
            a, ch, e = k // 6, k // 3 % 2, k % 3
            out[b, 8 * k : 8 * k + 8, ((a * 3 + b) * 3 + e) * 2 + ch] = 1
            e, a, ch = k // 6, k // 2 % 3, k % 2
            out[3 + b, 8 * k : 8 * k + 8, ((a * 3 + b) * 3 + e) * 2 + ch] = 1
    return out


def shards(frames, kspace, sens, mask, image, w_first, b_first, w_mid, b_mid, w_last):
    args = (
        kspace[0], sens, mask[0], image[0], jnp.asarray(dft_tables(), BF16), jnp.asarray(picks(), BF16),
        jnp.swapaxes(w_first, 3, 4).reshape(27, 2, CH), w_mid.reshape(27, CH, CH), w_last.reshape(27, 2, CH),
        b_first[None], b_mid[None],
    )
    dma = pltpu.SemaphoreType.DMA
    out = pl.pallas_call(
        functools.partial(kernel, frames),
        out_shape=pltpu.VMEM((RB, 2 * N), F32),
        in_specs=[pl.BlockSpec(memory_space=pl.ANY)] * len(args),
        out_specs=pl.BlockSpec(memory_space=pltpu.VMEM),
        scratch_shapes=[pltpu.VMEM(a.shape, a.dtype) for a in args]
        + [
            pltpu.VMEM((64, CH), F32),
            pltpu.VMEM((640, 144), BF16),
            pltpu.VMEM((3, 3 * CH, 3 * CH), BF16),
            pltpu.VMEM((144, 640), BF16),
            pltpu.VMEM((ROWS, 2 * N), BF16),
            pltpu.VMEM((NCO * RB, 2 * N), BF16),
            pltpu.VMEM((NCO, 2 * ROWS, N), BF16),
            pltpu.VMEM((NCO, ROWS, 2 * N), BF16),
            pltpu.VMEM((NCO, 2 * ROWS, N), BF16),
            pltpu.VMEM((ROWS, 2 * N), F32),
            pltpu.VMEM((GRP, 2 * HR, N), BF16),
            pltpu.VMEM((GRP, 2 * HR, N), BF16),
            pltpu.VMEM((ROWS + 16, 2 * N), F32),
            pltpu.VMEM((2 * HR, N), F32),
            pltpu.VMEM((5, 2 * HR, N), BF16),
            pltpu.VMEM((HR // 8, 5 * KF, N), BF16),
            pltpu.VMEM((3, 36 * CH, N), BF16),
            pltpu.VMEM((34 * CH, N), BF16),
            pltpu.VMEM((2, RB, 2 * N), BF16),
            pltpu.VMEM((2, RB, 2 * N), BF16),
            dma((len(args),)), dma((GRP,)), dma((GRP,)), dma((GRP,)), dma((GRP,)),
            dma((5,)), dma((5,)), dma((2,)), dma((2,)),
        ],
        compiler_params=pltpu.CompilerParams(
            collective_id=0, has_side_effects=True, vmem_limit_bytes=56 * 1024 * 1024
        ),
    )(*args)
    return out[None]


def solution(mesh):
    in_specs = (
        P("frame", "coil", None, None),
        P("coil", None, None),
        P("frame", "coil", None),
        P("frame", "coil", None),
        P(),
        P(),
        P(),
        P(),
        P(),
    )
    out_specs = P("frame", "coil", None)
    body = functools.partial(shards, mesh.shape["frame"])
    return jax.shard_map(body, mesh=mesh, in_specs=in_specs, out_specs=out_specs, check_vma=False)
```

```python
import functools

import jax
import jax.numpy as jnp
import numpy as np
from jax import lax
from jax.experimental import pallas as pl
from jax.experimental.pallas import tpu as pltpu
from jax.sharding import PartitionSpec as P

F32 = jnp.float32
BF16 = jnp.bfloat16
MESH = pl.DeviceIdType.MESH

ROWS = 256
N = 256
RB = 32
HR = 40
KF = 48
NCO = 8
CH = 64
GRP = 8


def dft_tables():
    idx = np.arange(N)
    ang = (idx[:, None] * idx[None, :] % N) * (2.0 * np.pi / N)
    fr = (np.cos(ang) / np.sqrt(N)).astype(np.float32)
    fi = (-np.sin(ang) / np.sqrt(N)).astype(np.float32)
    return np.stack([np.block([[fr, fi], [-fi, fr]]), np.block([[fr, -fi], [fi, fr]])])


def shift_right(v):
    lane = lax.broadcasted_iota(jnp.int32, v.shape, 1)
    return jnp.where(lane == 0, 0.0, pltpu.roll(v, 1, axis=1))


def shift_left(v):
    lane = lax.broadcasted_iota(jnp.int32, v.shape, 1)
    return jnp.where(lane == N - 1, 0.0, pltpu.roll(v, N - 1, axis=1))


def dot(a, b):
    return jnp.dot(a, b, preferred_element_type=F32)


def iota2(shape):
    return lax.broadcasted_iota(jnp.int32, shape, 0), lax.broadcasted_iota(jnp.int32, shape, 1)


def conv_weights(pick, wf, wm, wl, bf, bm, w54, w1, w2, w3):
    w54[...] = jnp.zeros((64, CH), F32)
    for k in range(27):
        w54[2 * k : 2 * k + 2, :] = wf[k].astype(F32)
    source = w54[...].astype(BF16)
    row, col = iota2((640, CH))
    tile = ((row & (CH - 1)) == col).astype(F32).astype(BF16)
    row, col = iota2((640, 144))
    base = jnp.where(row >= 512, (row >> 6) - 10, row >> 6)
    total = jnp.zeros((640, 144), F32)
    for b in range(3):
        z = dot(pick[b], source).astype(BF16)
        part = lax.dot_general(tile, z, (((1,), (1,)), ((), ())), preferred_element_type=F32)
        total = jnp.where((col & 7) == base + b, part, total)
    w1[...] = total.astype(BF16)
    for k in range(27):
        w54[2 * k : 2 * k + 2, :] = wl[k].astype(F32)
    source = w54[...].astype(BF16)
    row, col = iota2((CH, 640))
    tile = (row == (col & (CH - 1))).astype(F32).astype(BF16)
    row, col = iota2((144, 640))
    total = jnp.zeros((144, 640), F32)
    for b in range(3):
        z = dot(pick[3 + b], source).astype(BF16)
        total = jnp.where((col >> 6) == (row & 7) + b, dot(z, tile), total)
    w3[...] = total.astype(BF16)
    row, col = iota2((CH, 3 * CH))
    places = [(col == row + b * CH).astype(F32).astype(BF16) for b in range(3)]
    for a in range(3):
        for e in range(3):
            w2[a, e * CH : (e + 1) * CH, :] = sum(
                dot(wm[(a * 3 + b) * 3 + e], places[b]) for b in range(3)
            ).astype(BF16)
    return [jnp.broadcast_to(v[...], (N, CH)).T for v in (bf, bm)]


def kernel(
    frames,
    kspace_hbm, sens_hbm, mask_hbm, image_hbm, table_hbm, pick_hbm, wf_hbm, wm_hbm, wl_hbm, bf_hbm, bm_hbm,
    out_ref,
    ksp, sens, mask, image, table, pick, wf, wm, wl, bf, bm,
    w54, w1, w2, w3,
    xb, ci, cols, misfit, stacked, acc, gs, grecv, xr, xh, hb, kb, h1, h2, psend, precv,
    lsem, asend, arecv, bsend, brecv, csend, crecv, dsend, drecv,
):
    t = lax.axis_index("frame")
    j = lax.axis_index("coil")
    r0 = pl.multiple_of(j * RB, RB)

    loads = [
        pltpu.make_async_copy(src, dst, lsem.at[i])
        for i, (src, dst) in enumerate(
            [
                (image_hbm, image), (pick_hbm, pick), (wf_hbm, wf), (wm_hbm, wm), (wl_hbm, wl), (bf_hbm, bf),
                (bm_hbm, bm), (sens_hbm, sens), (table_hbm, table), (kspace_hbm, ksp), (mask_hbm, mask),
            ]
        )
    ]
    for c in loads:
        c.start()

    partners = [(d, (t + d >= 0) & (t + d < frames)) for d in (-2, 2, -1, 1)]

    barrier = pltpu.get_barrier_semaphore()
    for s in range(1, GRP):
        pl.semaphore_signal(barrier, inc=1, device_id={"coil": lax.rem(j + s, GRP)}, device_id_type=MESH)
    for d, here in partners:
        @pl.when(here)
        def _():
            pl.semaphore_signal(barrier, inc=1, device_id={"frame": t + d}, device_id_type=MESH)

    loads[0].wait()
    xb[pl.ds(r0, RB), :] = image[...].astype(BF16)
    for c in loads[1:7]:
        c.wait()
    bias1, bias2 = conv_weights(pick, wf, wm, wl, bf, bm, w54, w1, w2, w3)
    present = sum(here.astype(jnp.int32) for _, here in partners)
    pl.semaphore_wait(barrier, GRP - 1 + present)

    acopy = []
    for s in (4, 1, 7, 3, 5, 2, 6):
        c = pltpu.make_async_remote_copy(
            src_ref=xb.at[pl.ds(r0, RB)],
            dst_ref=xb.at[pl.ds(r0, RB)],
            send_sem=asend.at[s],
            recv_sem=arecv.at[s],
            device_id={"coil": lax.rem(j + s, GRP)},
            device_id_type=MESH,
        )
        c.start()
        acopy.append(c)

    loads[7].wait()
    loads[8].wait()

    def columns(shifts):
        for s in shifts:
            rq = pl.multiple_of(lax.rem(j - s + GRP, GRP) * RB, RB)
            xv = xb[pl.ds(rq, RB), :].astype(F32)
            x_re, x_im = xv[:, :N], xv[:, N:]
            for c in range(NCO):
                sv = sens[c, pl.ds(rq, RB), :].astype(F32)
                s_re, s_im = sv[:, :N], sv[:, N:]
                ci[s, c * RB : (c + 1) * RB, :N] = (s_re * x_re - s_im * x_im).astype(BF16)
                ci[s, c * RB : (c + 1) * RB, N:] = (s_re * x_im + s_im * x_re).astype(BF16)
        for s in shifts:
            rq = pl.multiple_of(lax.rem(j - s + GRP, GRP) * RB, RB)
            for half in range(2):
                spec = dot(ci[s], table[0, :, half * N : (half + 1) * N]).astype(BF16)
                for c in range(NCO):
                    cols[c, pl.ds(half * ROWS + rq, RB), :] = spec[c * RB : (c + 1) * RB]

    columns((0,))
    for shifts in ((4, 1, 7), (3, 5), (2, 6)):
        for s in shifts:
            pltpu.make_async_remote_copy(
                src_ref=xb.at[pl.ds(r0, RB)],
                dst_ref=xb.at[pl.ds(pl.multiple_of(lax.rem(j - s + GRP, GRP) * RB, RB), RB)],
                send_sem=asend.at[s],
                recv_sem=arecv.at[s],
                device_id={"coil": lax.rem(j + s, GRP)},
                device_id_type=MESH,
            ).wait_recv()
        columns(shifts)

    loads[9].wait()
    loads[10].wait()

    for c in range(NCO):
        for half in range(2):
            est = dot(table[1, half * ROWS : (half + 1) * ROWS, :], cols[c])
            k = ksp[c, :, half * N : (half + 1) * N].astype(F32)
            misfit[c, :, half * N : (half + 1) * N] = (est - k).astype(BF16)
    for c in range(NCO):
        for half in range(2):
            stacked[c, half * ROWS : (half + 1) * ROWS, :] = dot(
                misfit[c], table[1, :, half * N : (half + 1) * N]
            ).astype(BF16)
    def gradient(base):
        base = pl.multiple_of(base, 128)
        rows = pl.ds(base, 128)
        into = pl.ds(base + 8, 128)
        for c in range(NCO):
            m = mask[c : c + 1, :].astype(F32).astype(BF16)
            mm = jnp.concatenate([m, m], axis=1)
            b_re = dot(table[0, rows, :] * mm, stacked[c])
            b_im = dot(table[0, pl.ds(base + ROWS, 128), :] * mm, stacked[c])
            s_re, s_im = sens[c, rows, :N].astype(F32), sens[c, rows, N:].astype(F32)
            g_re = s_re * b_re + s_im * b_im
            g_im = s_re * b_im - s_im * b_re
            acc[into, :N] = g_re if c == 0 else acc[into, :N] + g_re
            acc[into, N:] = g_im if c == 0 else acc[into, N:] + g_im

    def haloed(q):
        v = acc[pl.ds(pl.multiple_of(q * RB, RB), HR + 8), :][5 : 5 + HR]
        return jnp.concatenate([v[:, :N], v[:, N:]], axis=0)

    bcopy = []

    def send(targets):
        begun = []
        for to in targets:
            slot = len(bcopy) + len(begun)
            gs[slot] = haloed(to).astype(BF16)
            s = lax.rem(to - j + GRP, GRP)
            begun.append(
                pltpu.make_async_remote_copy(
                    src_ref=gs.at[slot],
                    dst_ref=grecv.at[s],
                    send_sem=bsend.at[s],
                    recv_sem=brecv.at[s],
                    device_id={"coil": to},
                    device_id_type=MESH,
                )
            )
        for c in begun:
            c.start()
        bcopy.extend(begun)

    low = j < GRP // 2
    acc[:8, :] = jnp.zeros((8, 2 * N), F32)
    acc[ROWS + 8 :, :] = jnp.zeros((8, 2 * N), F32)
    gradient(jnp.where(low, 128, 0))
    send([jnp.where(low, 5, 0) + n for n in range(3)])
    gradient(jnp.where(low, 0, 128))
    start = jnp.where(low, 0, 3)
    send([start + lax.rem(j - start + n, 5) for n in range(1, 5)])

    xr[:ROWS, :] = pltpu.roll(xb[...].astype(F32), 3, axis=0)
    xr[ROWS:, :] = jnp.zeros((16, 2 * N), F32)
    for half in range(2):
        cut = slice(half * N, (half + 1) * N)
        xh[half * HR : (half + 1) * HR, :] = xr[pl.ds(r0, HR), cut]
        xh[half * HR + 3 : half * HR + 3 + RB, :] = image[:, cut]
    total = xh[...] - haloed(j)
    for c in bcopy:
        c.wait_recv()
    for s in range(1, GRP):
        total = total - grecv[s].astype(F32)
    line = lax.broadcasted_iota(jnp.int32, (2 * HR, N), 0)
    row = r0 - 3 + jnp.where(line >= HR, line - HR, line)
    total = jnp.where((row >= 0) & (row < ROWS), total, 0.0)
    xh[...] = total
    hb[2] = total.astype(BF16)

    for d, here in partners:
        def ccopy(d=d):
            return pltpu.make_async_remote_copy(
                src_ref=hb.at[2],
                dst_ref=hb.at[2 - d],
                send_sem=csend.at[d + 2],
                recv_sem=crecv.at[d + 2],
                device_id={"frame": t + d},
                device_id_type=MESH,
            )

        @pl.when(here)
        def _():
            ccopy().start()

        @pl.when(jnp.logical_not(here))
        def _():
            hb[2 + d] = jnp.zeros((2 * HR, N), BF16)

    def planes(f):
        v = hb[f].astype(F32)
        parts = []
        for half in range(2):
            p = v[half * HR : (half + 1) * HR]
            parts += [shift_right(p), p, shift_left(p)]
        for i in range(HR // 8):
            kb[i, f * KF : (f + 1) * KF, :] = jnp.concatenate(
                [p[8 * i : 8 * i + 8] for p in parts], axis=0
            ).astype(BF16)

    def arrived(d):
        @pl.when((t + d >= 0) & (t + d < frames))
        def _():
            pltpu.make_async_remote_copy(
                src_ref=hb.at[2],
                dst_ref=hb.at[2 + d],
                send_sem=csend.at[2 - d],
                recv_sem=crecv.at[2 - d],
                device_id={"frame": t + d},
                device_id_type=MESH,
            ).wait_recv()

        planes(2 + d)

    def first(f):
        def put(q, v):
            h1[f, q * CH : (q + 1) * CH, :] = jnp.maximum(v + bias1, 0.0).astype(BF16)

        for i in range(5):
            here_k = kb[i, f * KF : (f + 3) * KF, :]
            if i == 4:
                top = dot(w1[: 4 * CH, :], here_k)
                for q in range(4):
                    put(32 + q, top[q * CH : (q + 1) * CH])
                continue
            next_k = kb[i + 1, f * KF : (f + 3) * KF, :]
            top = dot(w1[: 6 * CH, :], here_k)
            low = dot(w1[6 * CH : 8 * CH, :], here_k) + dot(w1[8 * CH :, :], next_k)
            for q in range(6):
                put(8 * i + q, top[q * CH : (q + 1) * CH])
            for q in range(2):
                put(8 * i + 6 + q, low[q * CH : (q + 1) * CH])

    planes(2)
    arrived(-1)
    arrived(1)
    first(1)
    arrived(-2)
    first(0)
    arrived(2)
    first(2)

    @pl.when(j == 0)
    def _():
        h1[:, : 2 * CH, :] = jnp.zeros((3, 2 * CH, N), BF16)

    @pl.when(j == GRP - 1)
    def _():
        h1[:, 34 * CH :, :] = jnp.zeros((3, 2 * CH, N), BF16)

    @pl.when(t == 0)
    def _():
        h1[0] = jnp.zeros((36 * CH, N), BF16)

    @pl.when(t == frames - 1)
    def _():
        h1[2] = jnp.zeros((36 * CH, N), BF16)

    for r in range(34):
        base = r * CH
        taps = dot(w2[0], h1[0, base : base + 3 * CH, :])
        taps += dot(w2[1], h1[1, base : base + 3 * CH, :])
        taps += dot(w2[2], h1[2, base : base + 3 * CH, :])
        v = taps[CH : 2 * CH] + shift_right(taps[:CH]) + shift_left(taps[2 * CH :]) + bias2
        h2[base : base + CH, :] = jnp.maximum(v, 0.0).astype(BF16)

    @pl.when(j == 0)
    def _():
        h2[:CH, :] = jnp.zeros((CH, N), BF16)

    @pl.when(j == GRP - 1)
    def _():
        h2[33 * CH :, :] = jnp.zeros((CH, N), BF16)

    blocks = []
    for i in range(RB // 8):
        base = i * 8 * CH
        taps = dot(w3[...], h2[base : base + 10 * CH, :])
        blocks.append(taps[48:96] + shift_right(taps[:48]) + shift_left(taps[96:]))
    for a in (0, 2, 1):
        for half in range(2):
            o = (a * 2 + half) * 8
            v = jnp.concatenate([b[o : o + 8] for b in blocks], axis=0)
            cut = slice(half * N, (half + 1) * N)
            if a == 1:
                xh[half * HR + 3 : half * HR + 3 + RB, :] += v
            else:
                psend[a // 2, :, cut] = v.astype(BF16)

    ends = [(1, 0, t + 1 < frames), (-1, 1, t >= 1)]
    for n, (d, a, here) in enumerate(ends):
        @pl.when(here)
        def _():
            pltpu.make_async_remote_copy(
                src_ref=psend.at[a],
                dst_ref=precv.at[n],
                send_sem=dsend.at[n],
                recv_sem=drecv.at[n],
                device_id={"frame": t + d},
                device_id_type=MESH,
            ).start()

    for half in range(2):
        out_ref[:, half * N : (half + 1) * N] = xh[half * HR + 3 : half * HR + 3 + RB, :]
    for n, (d, a, here) in enumerate(ends):
        @pl.when((t - d >= 0) & (t - d < frames))
        def _():
            pltpu.make_async_remote_copy(
                src_ref=psend.at[a],
                dst_ref=precv.at[n],
                send_sem=dsend.at[n],
                recv_sem=drecv.at[n],
                device_id={"frame": t - d},
                device_id_type=MESH,
            ).wait_recv()
            out_ref[...] += precv[n].astype(F32)

    for c in acopy + bcopy:
        c.wait_send()
    for d, here in partners:
        @pl.when(here)
        def _():
            pltpu.make_async_remote_copy(
                src_ref=hb.at[2],
                dst_ref=hb.at[2 - d],
                send_sem=csend.at[d + 2],
                recv_sem=crecv.at[d + 2],
                device_id={"frame": t + d},
                device_id_type=MESH,
            ).wait_send()
    for n, (d, a, here) in enumerate(ends):
        @pl.when(here)
        def _():
            pltpu.make_async_remote_copy(
                src_ref=psend.at[a],
                dst_ref=precv.at[n],
                send_sem=dsend.at[n],
                recv_sem=drecv.at[n],
                device_id={"frame": t + d},
                device_id_type=MESH,
            ).wait_send()


def picks():
    out = np.zeros((6, 144, 64), np.float32)
    for b in range(3):
        for k in range(18):
            a, ch, e = k // 6, k // 3 % 2, k % 3
            out[b, 8 * k : 8 * k + 8, ((a * 3 + b) * 3 + e) * 2 + ch] = 1
            e, a, ch = k // 6, k // 2 % 3, k % 2
            out[3 + b, 8 * k : 8 * k + 8, ((a * 3 + b) * 3 + e) * 2 + ch] = 1
    return out


def shards(frames, kspace, sens, mask, image, w_first, b_first, w_mid, b_mid, w_last):
    args = (
        kspace[0], sens, mask[0], image[0], jnp.asarray(dft_tables(), BF16), jnp.asarray(picks(), BF16),
        jnp.swapaxes(w_first, 3, 4).reshape(27, 2, CH), w_mid.reshape(27, CH, CH), w_last.reshape(27, 2, CH),
        b_first[None], b_mid[None],
    )
    dma = pltpu.SemaphoreType.DMA
    out = pl.pallas_call(
        functools.partial(kernel, frames),
        out_shape=pltpu.VMEM((RB, 2 * N), F32),
        in_specs=[pl.BlockSpec(memory_space=pl.ANY)] * len(args),
        out_specs=pl.BlockSpec(memory_space=pltpu.VMEM),
        scratch_shapes=[pltpu.VMEM(a.shape, a.dtype) for a in args]
        + [
            pltpu.VMEM((64, CH), F32),
            pltpu.VMEM((640, 144), BF16),
            pltpu.VMEM((3, 3 * CH, 3 * CH), BF16),
            pltpu.VMEM((144, 640), BF16),
            pltpu.VMEM((ROWS, 2 * N), BF16),
            pltpu.VMEM((GRP, NCO * RB, 2 * N), BF16),
            pltpu.VMEM((NCO, 2 * ROWS, N), BF16),
            pltpu.VMEM((NCO, ROWS, 2 * N), BF16),
            pltpu.VMEM((NCO, 2 * ROWS, N), BF16),
            pltpu.VMEM((ROWS + 16, 2 * N), F32),
            pltpu.VMEM((GRP, 2 * HR, N), BF16),
            pltpu.VMEM((GRP, 2 * HR, N), BF16),
            pltpu.VMEM((ROWS + 16, 2 * N), F32),
            pltpu.VMEM((2 * HR, N), F32),
            pltpu.VMEM((5, 2 * HR, N), BF16),
            pltpu.VMEM((HR // 8, 5 * KF, N), BF16),
            pltpu.VMEM((3, 36 * CH, N), BF16),
            pltpu.VMEM((34 * CH, N), BF16),
            pltpu.VMEM((2, RB, 2 * N), BF16),
            pltpu.VMEM((2, RB, 2 * N), BF16),
            dma((len(args),)), dma((GRP,)), dma((GRP,)), dma((GRP,)), dma((GRP,)),
            dma((5,)), dma((5,)), dma((2,)), dma((2,)),
        ],
        compiler_params=pltpu.CompilerParams(
            collective_id=0, has_side_effects=True, vmem_limit_bytes=56 * 1024 * 1024
        ),
    )(*args)
    return out[None]


def solution(mesh):
    in_specs = (
        P("frame", "coil", None, None),
        P("coil", None, None),
        P("frame", "coil", None),
        P("frame", "coil", None),
        P(),
        P(),
        P(),
        P(),
        P(),
    )
    out_specs = P("frame", "coil", None)
    body = functools.partial(shards, mesh.shape["frame"])
    return jax.shard_map(body, mesh=mesh, in_specs=in_specs, out_specs=out_specs, check_vma=False)
```

```python
import functools

import jax
import jax.numpy as jnp
import numpy as np
from jax import lax
from jax.experimental import pallas as pl
from jax.experimental.pallas import tpu as pltpu
from jax.sharding import PartitionSpec as P

F32 = jnp.float32
BF16 = jnp.bfloat16
MESH = pl.DeviceIdType.MESH

ROWS = 256
N = 256
RB = 32
HR = 40
KF = 48
NCO = 8
CH = 64
GRP = 8


def dft_tables():
    idx = np.arange(N)
    ang = (idx[:, None] * idx[None, :] % N) * (2.0 * np.pi / N)
    fr = (np.cos(ang) / np.sqrt(N)).astype(np.float32)
    fi = (-np.sin(ang) / np.sqrt(N)).astype(np.float32)
    return np.stack([np.block([[fr, fi], [-fi, fr]]), np.block([[fr, -fi], [fi, fr]])])


def shift_right(v):
    lane = lax.broadcasted_iota(jnp.int32, v.shape, 1)
    return jnp.where(lane == 0, 0.0, pltpu.roll(v, 1, axis=1))


def shift_left(v):
    lane = lax.broadcasted_iota(jnp.int32, v.shape, 1)
    return jnp.where(lane == N - 1, 0.0, pltpu.roll(v, N - 1, axis=1))


def dot(a, b):
    return jnp.dot(a, b, preferred_element_type=F32)


def iota2(shape):
    return lax.broadcasted_iota(jnp.int32, shape, 0), lax.broadcasted_iota(jnp.int32, shape, 1)


def first_weights(pick, wf, w54, w1):
    w54[...] = jnp.zeros((64, CH), F32)
    for k in range(27):
        w54[2 * k : 2 * k + 2, :] = wf[k].astype(F32)
    source = w54[...].astype(BF16)
    row, col = iota2((640, CH))
    tile = ((row & (CH - 1)) == col).astype(F32).astype(BF16)
    row, col = iota2((640, 144))
    base = jnp.where(row >= 512, (row >> 6) - 10, row >> 6)
    total = jnp.zeros((640, 144), F32)
    for b in range(3):
        z = dot(pick[b], source).astype(BF16)
        part = lax.dot_general(tile, z, (((1,), (1,)), ((), ())), preferred_element_type=F32)
        total = jnp.where((col & 7) == base + b, part, total)
    w1[...] = total.astype(BF16)


def other_weights(pick, wm, wl, bf, bm, w54, w2, w3):
    for k in range(27):
        w54[2 * k : 2 * k + 2, :] = wl[k].astype(F32)
    source = w54[...].astype(BF16)
    row, col = iota2((CH, 640))
    tile = (row == (col & (CH - 1))).astype(F32).astype(BF16)
    row, col = iota2((144, 640))
    total = jnp.zeros((144, 640), F32)
    for b in range(3):
        z = dot(pick[3 + b], source).astype(BF16)
        total = jnp.where((col >> 6) == (row & 7) + b, dot(z, tile), total)
    w3[...] = total.astype(BF16)
    row, col = iota2((CH, 3 * CH))
    places = [(col == row + b * CH).astype(F32).astype(BF16) for b in range(3)]
    for a in range(3):
        for e in range(3):
            w2[a, e * CH : (e + 1) * CH, :] = sum(
                dot(wm[(a * 3 + b) * 3 + e], places[b]) for b in range(3)
            ).astype(BF16)
    return [jnp.broadcast_to(v[...], (N, CH)).T for v in (bf, bm)]


def kernel(
    frames,
    kspace_hbm, sens_hbm, mask_hbm, image_hbm, table_hbm, pick_hbm, wf_hbm, wm_hbm, wl_hbm, bf_hbm, bm_hbm,
    out_ref,
    ksp, sens, mask, image, table, pick, wf, wm, wl, bf, bm,
    w54, w1, w2, w3,
    xb, ci, cols, misfit, stacked, acc, gs, grecv, xr, xh, hb, kb, h1, h2, psend, precv,
    lsem, asend, arecv, bsend, brecv, csend, crecv, dsend, drecv,
):
    t = lax.axis_index("frame")
    j = lax.axis_index("coil")
    r0 = pl.multiple_of(j * RB, RB)

    loads = [
        pltpu.make_async_copy(src, dst, lsem.at[i])
        for i, (src, dst) in enumerate(
            [
                (image_hbm, image), (pick_hbm, pick), (wf_hbm, wf), (wm_hbm, wm), (wl_hbm, wl), (bf_hbm, bf),
                (bm_hbm, bm), (sens_hbm, sens), (table_hbm, table), (kspace_hbm, ksp), (mask_hbm, mask),
            ]
        )
    ]
    for c in loads:
        c.start()

    partners = [(d, (t + d >= 0) & (t + d < frames)) for d in (-2, 2, -1, 1)]

    barrier = pltpu.get_barrier_semaphore()
    for s in range(1, GRP):
        pl.semaphore_signal(barrier, inc=1, device_id={"coil": lax.rem(j + s, GRP)}, device_id_type=MESH)
    for d, here in partners:
        @pl.when(here)
        def _():
            pl.semaphore_signal(barrier, inc=1, device_id={"frame": t + d}, device_id_type=MESH)

    loads[0].wait()
    xb[pl.ds(r0, RB), :] = image[...].astype(BF16)
    for c in loads[1:7]:
        c.wait()
    first_weights(pick, wf, w54, w1)
    present = sum(here.astype(jnp.int32) for _, here in partners)
    pl.semaphore_wait(barrier, GRP - 1 + present)

    acopy = []
    for s in (4, 1, 7, 3, 5, 2, 6):
        c = pltpu.make_async_remote_copy(
            src_ref=xb.at[pl.ds(r0, RB)],
            dst_ref=xb.at[pl.ds(r0, RB)],
            send_sem=asend.at[s],
            recv_sem=arecv.at[s],
            device_id={"coil": lax.rem(j + s, GRP)},
            device_id_type=MESH,
        )
        c.start()
        acopy.append(c)

    loads[7].wait()
    loads[8].wait()

    def columns(shifts):
        for s in shifts:
            rq = pl.multiple_of(lax.rem(j - s + GRP, GRP) * RB, RB)
            xv = xb[pl.ds(rq, RB), :].astype(F32)
            x_re, x_im = xv[:, :N], xv[:, N:]
            for c in range(NCO):
                sv = sens[c, pl.ds(rq, RB), :].astype(F32)
                s_re, s_im = sv[:, :N], sv[:, N:]
                ci[s, c * RB : (c + 1) * RB, :N] = (s_re * x_re - s_im * x_im).astype(BF16)
                ci[s, c * RB : (c + 1) * RB, N:] = (s_re * x_im + s_im * x_re).astype(BF16)
        for s in shifts:
            rq = pl.multiple_of(lax.rem(j - s + GRP, GRP) * RB, RB)
            for half in range(2):
                spec = dot(ci[s], table[0, :, half * N : (half + 1) * N]).astype(BF16)
                for c in range(NCO):
                    cols[c, pl.ds(half * ROWS + rq, RB), :] = spec[c * RB : (c + 1) * RB]

    columns((0,))
    for shifts in ((4, 1, 7), (3, 5), (2, 6)):
        for s in shifts:
            pltpu.make_async_remote_copy(
                src_ref=xb.at[pl.ds(r0, RB)],
                dst_ref=xb.at[pl.ds(pl.multiple_of(lax.rem(j - s + GRP, GRP) * RB, RB), RB)],
                send_sem=asend.at[s],
                recv_sem=arecv.at[s],
                device_id={"coil": lax.rem(j + s, GRP)},
                device_id_type=MESH,
            ).wait_recv()
        columns(shifts)

    loads[9].wait()
    loads[10].wait()

    for c in range(NCO):
        for half in range(2):
            est = dot(table[1, half * ROWS : (half + 1) * ROWS, :], cols[c])
            k = ksp[c, :, half * N : (half + 1) * N].astype(F32)
            misfit[c, :, half * N : (half + 1) * N] = (est - k).astype(BF16)
    for c in range(NCO):
        for half in range(2):
            stacked[c, half * ROWS : (half + 1) * ROWS, :] = dot(
                misfit[c], table[1, :, half * N : (half + 1) * N]
            ).astype(BF16)
    def gradient(base):
        base = pl.multiple_of(base, 128)
        rows = pl.ds(base, 128)
        into = pl.ds(base + 8, 128)
        for c in range(NCO):
            m = mask[c : c + 1, :].astype(F32).astype(BF16)
            mm = jnp.concatenate([m, m], axis=1)
            b_re = dot(table[0, rows, :] * mm, stacked[c])
            b_im = dot(table[0, pl.ds(base + ROWS, 128), :] * mm, stacked[c])
            s_re, s_im = sens[c, rows, :N].astype(F32), sens[c, rows, N:].astype(F32)
            g_re = s_re * b_re + s_im * b_im
            g_im = s_re * b_im - s_im * b_re
            acc[into, :N] = g_re if c == 0 else acc[into, :N] + g_re
            acc[into, N:] = g_im if c == 0 else acc[into, N:] + g_im

    def haloed(q):
        v = acc[pl.ds(pl.multiple_of(q * RB, RB), HR + 8), :][5 : 5 + HR]
        return jnp.concatenate([v[:, :N], v[:, N:]], axis=0)

    bcopy = []

    def send(targets):
        begun = []
        for to in targets:
            slot = len(bcopy) + len(begun)
            gs[slot] = haloed(to).astype(BF16)
            s = lax.rem(to - j + GRP, GRP)
            begun.append(
                pltpu.make_async_remote_copy(
                    src_ref=gs.at[slot],
                    dst_ref=grecv.at[s],
                    send_sem=bsend.at[s],
                    recv_sem=brecv.at[s],
                    device_id={"coil": to},
                    device_id_type=MESH,
                )
            )
            if len(begun) > 1:
                begun[-2].start()
        begun[-1].start()
        bcopy.extend(begun)

    low = j < GRP // 2
    acc[:8, :] = jnp.zeros((8, 2 * N), F32)
    acc[ROWS + 8 :, :] = jnp.zeros((8, 2 * N), F32)
    gradient(jnp.where(low, 128, 0))
    send([jnp.where(low, 5, 0) + n for n in range(3)])
    gradient(jnp.where(low, 0, 128))
    start = jnp.where(low, 0, 3)
    send([start + lax.rem(j - start + n, 5) for n in range(1, 5)])

    xr[:ROWS, :] = pltpu.roll(xb[...].astype(F32), 3, axis=0)
    xr[ROWS:, :] = jnp.zeros((16, 2 * N), F32)
    for half in range(2):
        cut = slice(half * N, (half + 1) * N)
        xh[half * HR : (half + 1) * HR, :] = xr[pl.ds(r0, HR), cut]
        xh[half * HR + 3 : half * HR + 3 + RB, :] = image[:, cut]
    total = xh[...] - haloed(j)
    bias1, bias2 = other_weights(pick, wm, wl, bf, bm, w54, w2, w3)
    for s in (4, 3, 5, 2, 6, 1, 7):
        pltpu.make_async_remote_copy(
            src_ref=gs.at[0],
            dst_ref=grecv.at[s],
            send_sem=bsend.at[s],
            recv_sem=brecv.at[s],
            device_id={"coil": lax.rem(j + s, GRP)},
            device_id_type=MESH,
        ).wait_recv()
        total = total - grecv[s].astype(F32)
    line = lax.broadcasted_iota(jnp.int32, (2 * HR, N), 0)
    row = r0 - 3 + jnp.where(line >= HR, line - HR, line)
    total = jnp.where((row >= 0) & (row < ROWS), total, 0.0)
    xh[...] = total
    hb[2] = total.astype(BF16)

    for d, here in partners:
        def ccopy(d=d):
            return pltpu.make_async_remote_copy(
                src_ref=hb.at[2],
                dst_ref=hb.at[2 - d],
                send_sem=csend.at[d + 2],
                recv_sem=crecv.at[d + 2],
                device_id={"frame": t + d},
                device_id_type=MESH,
            )

        @pl.when(here)
        def _():
            ccopy().start()

        @pl.when(jnp.logical_not(here))
        def _():
            hb[2 + d] = jnp.zeros((2 * HR, N), BF16)

    def planes(f):
        v = hb[f].astype(F32)
        parts = []
        for half in range(2):
            p = v[half * HR : (half + 1) * HR]
            parts += [shift_right(p), p, shift_left(p)]
        for i in range(HR // 8):
            kb[i, f * KF : (f + 1) * KF, :] = jnp.concatenate(
                [p[8 * i : 8 * i + 8] for p in parts], axis=0
            ).astype(BF16)

    def arrived(d):
        @pl.when((t + d >= 0) & (t + d < frames))
        def _():
            pltpu.make_async_remote_copy(
                src_ref=hb.at[2],
                dst_ref=hb.at[2 + d],
                send_sem=csend.at[2 - d],
                recv_sem=crecv.at[2 - d],
                device_id={"frame": t + d},
                device_id_type=MESH,
            ).wait_recv()

        planes(2 + d)

    def first(f):
        def put(q, v):
            h1[f, q * CH : (q + 1) * CH, :] = jnp.maximum(v + bias1, 0.0).astype(BF16)

        for i in range(5):
            here_k = kb[i, f * KF : (f + 3) * KF, :]
            if i == 4:
                top = dot(w1[: 4 * CH, :], here_k)
                for q in range(4):
                    put(32 + q, top[q * CH : (q + 1) * CH])
                continue
            next_k = kb[i + 1, f * KF : (f + 3) * KF, :]
            top = dot(w1[: 6 * CH, :], here_k)
            low = dot(w1[6 * CH : 8 * CH, :], here_k) + dot(w1[8 * CH :, :], next_k)
            for q in range(6):
                put(8 * i + q, top[q * CH : (q + 1) * CH])
            for q in range(2):
                put(8 * i + 6 + q, low[q * CH : (q + 1) * CH])

    planes(2)
    arrived(-1)
    arrived(1)
    first(1)
    arrived(-2)
    first(0)
    arrived(2)
    first(2)

    @pl.when(j == 0)
    def _():
        h1[:, : 2 * CH, :] = jnp.zeros((3, 2 * CH, N), BF16)

    @pl.when(j == GRP - 1)
    def _():
        h1[:, 34 * CH :, :] = jnp.zeros((3, 2 * CH, N), BF16)

    @pl.when(t == 0)
    def _():
        h1[0] = jnp.zeros((36 * CH, N), BF16)

    @pl.when(t == frames - 1)
    def _():
        h1[2] = jnp.zeros((36 * CH, N), BF16)

    for r in range(34):
        base = r * CH
        taps = dot(w2[0], h1[0, base : base + 3 * CH, :])
        taps += dot(w2[1], h1[1, base : base + 3 * CH, :])
        taps += dot(w2[2], h1[2, base : base + 3 * CH, :])
        v = taps[CH : 2 * CH] + shift_right(taps[:CH]) + shift_left(taps[2 * CH :]) + bias2
        h2[base : base + CH, :] = jnp.maximum(v, 0.0).astype(BF16)

    @pl.when(j == 0)
    def _():
        h2[:CH, :] = jnp.zeros((CH, N), BF16)

    @pl.when(j == GRP - 1)
    def _():
        h2[33 * CH :, :] = jnp.zeros((CH, N), BF16)

    blocks = []
    for i in range(RB // 8):
        base = i * 8 * CH
        taps = dot(w3[...], h2[base : base + 10 * CH, :])
        blocks.append(taps[48:96] + shift_right(taps[:48]) + shift_left(taps[96:]))
    for a in (0, 2, 1):
        for half in range(2):
            o = (a * 2 + half) * 8
            v = jnp.concatenate([b[o : o + 8] for b in blocks], axis=0)
            cut = slice(half * N, (half + 1) * N)
            if a == 1:
                xh[half * HR + 3 : half * HR + 3 + RB, :] += v
            else:
                psend[a // 2, :, cut] = v.astype(BF16)

    ends = [(1, 0, t + 1 < frames), (-1, 1, t >= 1)]
    for n, (d, a, here) in enumerate(ends):
        @pl.when(here)
        def _():
            pltpu.make_async_remote_copy(
                src_ref=psend.at[a],
                dst_ref=precv.at[n],
                send_sem=dsend.at[n],
                recv_sem=drecv.at[n],
                device_id={"frame": t + d},
                device_id_type=MESH,
            ).start()

    for half in range(2):
        out_ref[:, half * N : (half + 1) * N] = xh[half * HR + 3 : half * HR + 3 + RB, :]
    for n, (d, a, here) in enumerate(ends):
        @pl.when((t - d >= 0) & (t - d < frames))
        def _():
            pltpu.make_async_remote_copy(
                src_ref=psend.at[a],
                dst_ref=precv.at[n],
                send_sem=dsend.at[n],
                recv_sem=drecv.at[n],
                device_id={"frame": t - d},
                device_id_type=MESH,
            ).wait_recv()
            out_ref[...] += precv[n].astype(F32)

    for c in acopy + bcopy:
        c.wait_send()
    for d, here in partners:
        @pl.when(here)
        def _():
            pltpu.make_async_remote_copy(
                src_ref=hb.at[2],
                dst_ref=hb.at[2 - d],
                send_sem=csend.at[d + 2],
                recv_sem=crecv.at[d + 2],
                device_id={"frame": t + d},
                device_id_type=MESH,
            ).wait_send()
    for n, (d, a, here) in enumerate(ends):
        @pl.when(here)
        def _():
            pltpu.make_async_remote_copy(
                src_ref=psend.at[a],
                dst_ref=precv.at[n],
                send_sem=dsend.at[n],
                recv_sem=drecv.at[n],
                device_id={"frame": t + d},
                device_id_type=MESH,
            ).wait_send()


def picks():
    out = np.zeros((6, 144, 64), np.float32)
    for b in range(3):
        for k in range(18):
            a, ch, e = k // 6, k // 3 % 2, k % 3
            out[b, 8 * k : 8 * k + 8, ((a * 3 + b) * 3 + e) * 2 + ch] = 1
            e, a, ch = k // 6, k // 2 % 3, k % 2
            out[3 + b, 8 * k : 8 * k + 8, ((a * 3 + b) * 3 + e) * 2 + ch] = 1
    return out


def shards(frames, kspace, sens, mask, image, w_first, b_first, w_mid, b_mid, w_last):
    args = (
        kspace[0], sens, mask[0], image[0], jnp.asarray(dft_tables(), BF16), jnp.asarray(picks(), BF16),
        jnp.swapaxes(w_first, 3, 4).reshape(27, 2, CH), w_mid.reshape(27, CH, CH), w_last.reshape(27, 2, CH),
        b_first[None], b_mid[None],
    )
    dma = pltpu.SemaphoreType.DMA
    out = pl.pallas_call(
        functools.partial(kernel, frames),
        out_shape=pltpu.VMEM((RB, 2 * N), F32),
        in_specs=[pl.BlockSpec(memory_space=pl.ANY)] * len(args),
        out_specs=pl.BlockSpec(memory_space=pltpu.VMEM),
        scratch_shapes=[pltpu.VMEM(a.shape, a.dtype) for a in args]
        + [
            pltpu.VMEM((64, CH), F32),
            pltpu.VMEM((640, 144), BF16),
            pltpu.VMEM((3, 3 * CH, 3 * CH), BF16),
            pltpu.VMEM((144, 640), BF16),
            pltpu.VMEM((ROWS, 2 * N), BF16),
            pltpu.VMEM((GRP, NCO * RB, 2 * N), BF16),
            pltpu.VMEM((NCO, 2 * ROWS, N), BF16),
            pltpu.VMEM((NCO, ROWS, 2 * N), BF16),
            pltpu.VMEM((NCO, 2 * ROWS, N), BF16),
            pltpu.VMEM((ROWS + 16, 2 * N), F32),
            pltpu.VMEM((GRP, 2 * HR, N), BF16),
            pltpu.VMEM((GRP, 2 * HR, N), BF16),
            pltpu.VMEM((ROWS + 16, 2 * N), F32),
            pltpu.VMEM((2 * HR, N), F32),
            pltpu.VMEM((5, 2 * HR, N), BF16),
            pltpu.VMEM((HR // 8, 5 * KF, N), BF16),
            pltpu.VMEM((3, 36 * CH, N), BF16),
            pltpu.VMEM((34 * CH, N), BF16),
            pltpu.VMEM((2, RB, 2 * N), BF16),
            pltpu.VMEM((2, RB, 2 * N), BF16),
            dma((len(args),)), dma((GRP,)), dma((GRP,)), dma((GRP,)), dma((GRP,)),
            dma((5,)), dma((5,)), dma((2,)), dma((2,)),
        ],
        compiler_params=pltpu.CompilerParams(
            collective_id=0, has_side_effects=True, vmem_limit_bytes=56 * 1024 * 1024
        ),
    )(*args)
    return out[None]


def solution(mesh):
    in_specs = (
        P("frame", "coil", None, None),
        P("coil", None, None),
        P("frame", "coil", None),
        P("frame", "coil", None),
        P(),
        P(),
        P(),
        P(),
        P(),
    )
    out_specs = P("frame", "coil", None)
    body = functools.partial(shards, mesh.shape["frame"])
    return jax.shard_map(body, mesh=mesh, in_specs=in_specs, out_specs=out_specs, check_vma=False)
```

```python
import functools

import jax
import jax.numpy as jnp
import numpy as np
from jax import lax
from jax.experimental import pallas as pl
from jax.experimental.pallas import tpu as pltpu
from jax.sharding import PartitionSpec as P

F32 = jnp.float32
BF16 = jnp.bfloat16
MESH = pl.DeviceIdType.MESH

ROWS = 256
N = 256
RB = 32
HR = 40
KF = 48
NCO = 8
CH = 64
GRP = 8


def dft_tables():
    idx = np.arange(N)
    ang = (idx[:, None] * idx[None, :] % N) * (2.0 * np.pi / N)
    fr = (np.cos(ang) / np.sqrt(N)).astype(np.float32)
    fi = (-np.sin(ang) / np.sqrt(N)).astype(np.float32)
    return np.stack([np.block([[fr, fi], [-fi, fr]]), np.block([[fr, -fi], [fi, fr]])])


def shift_right(v):
    lane = lax.broadcasted_iota(jnp.int32, v.shape, 1)
    return jnp.where(lane == 0, 0.0, pltpu.roll(v, 1, axis=1))


def shift_left(v):
    lane = lax.broadcasted_iota(jnp.int32, v.shape, 1)
    return jnp.where(lane == N - 1, 0.0, pltpu.roll(v, N - 1, axis=1))


def dot(a, b):
    return jnp.dot(a, b, preferred_element_type=F32)


def iota2(shape):
    return lax.broadcasted_iota(jnp.int32, shape, 0), lax.broadcasted_iota(jnp.int32, shape, 1)


def first_weights(pick, wf, w54, w1):
    w54[...] = jnp.zeros((64, CH), F32)
    for k in range(27):
        w54[2 * k : 2 * k + 2, :] = wf[k].astype(F32)
    source = w54[...].astype(BF16)
    row, col = iota2((640, CH))
    tile = ((row & (CH - 1)) == col).astype(F32).astype(BF16)
    row, col = iota2((640, 144))
    base = jnp.where(row >= 512, (row >> 6) - 10, row >> 6)
    total = jnp.zeros((640, 144), F32)
    for b in range(3):
        z = dot(pick[b], source).astype(BF16)
        part = lax.dot_general(tile, z, (((1,), (1,)), ((), ())), preferred_element_type=F32)
        total = jnp.where((col & 7) == base + b, part, total)
    w1[...] = total.astype(BF16)


def other_weights(pick, wm, wl, bf, bm, w54, w2, w3):
    for k in range(27):
        w54[2 * k : 2 * k + 2, :] = wl[k].astype(F32)
    source = w54[...].astype(BF16)
    row, col = iota2((CH, 640))
    tile = (row == (col & (CH - 1))).astype(F32).astype(BF16)
    row, col = iota2((144, 640))
    total = jnp.zeros((144, 640), F32)
    for b in range(3):
        z = dot(pick[3 + b], source).astype(BF16)
        total = jnp.where((col >> 6) == (row & 7) + b, dot(z, tile), total)
    w3[...] = total.astype(BF16)
    row, col = iota2((CH, 3 * CH))
    places = [(col == row + b * CH).astype(F32).astype(BF16) for b in range(3)]
    for a in range(3):
        for e in range(3):
            w2[a, e * CH : (e + 1) * CH, :] = sum(
                dot(wm[(a * 3 + b) * 3 + e], places[b]) for b in range(3)
            ).astype(BF16)
    return [jnp.broadcast_to(v[...], (N, CH)).T for v in (bf, bm)]


def kernel(
    frames,
    kspace_hbm, sens_hbm, mask_hbm, image_hbm, table_hbm, pick_hbm, wf_hbm, wm_hbm, wl_hbm, bf_hbm, bm_hbm,
    out_ref,
    ksp, sens, mask, image, table, pick, wf, wm, wl, bf, bm,
    w54, w1, w2, w3,
    xb, ci, cols, misfit, stacked, acc, gs, grecv, xr, xh, hb, kb, h1, h2, psend, precv,
    lsem, asend, arecv, bsend, brecv, csend, crecv, dsend, drecv,
):
    t = lax.axis_index("frame")
    j = lax.axis_index("coil")
    r0 = pl.multiple_of(j * RB, RB)

    loads = [
        pltpu.make_async_copy(src, dst, lsem.at[i])
        for i, (src, dst) in enumerate(
            [
                (image_hbm, image), (pick_hbm, pick), (wf_hbm, wf), (wm_hbm, wm), (wl_hbm, wl), (bf_hbm, bf),
                (bm_hbm, bm), (sens_hbm, sens), (table_hbm, table), (kspace_hbm, ksp), (mask_hbm, mask),
            ]
        )
    ]
    for c in loads:
        c.start()

    partners = [(d, (t + d >= 0) & (t + d < frames)) for d in (-1, 1, -2, 2)]

    barrier = pltpu.get_barrier_semaphore()
    for s in range(1, GRP):
        pl.semaphore_signal(barrier, inc=1, device_id={"coil": lax.rem(j + s, GRP)}, device_id_type=MESH)
    for d, here in partners:
        @pl.when(here)
        def _():
            pl.semaphore_signal(barrier, inc=1, device_id={"frame": t + d}, device_id_type=MESH)

    loads[0].wait()
    xb[pl.ds(r0, RB), :] = image[...].astype(BF16)
    for c in loads[1:7]:
        c.wait()
    first_weights(pick, wf, w54, w1)
    present = sum(here.astype(jnp.int32) for _, here in partners)
    pl.semaphore_wait(barrier, GRP - 1 + present)

    acopy = []
    for s in (4, 1, 7, 3, 5, 2, 6):
        c = pltpu.make_async_remote_copy(
            src_ref=xb.at[pl.ds(r0, RB)],
            dst_ref=xb.at[pl.ds(r0, RB)],
            send_sem=asend.at[s],
            recv_sem=arecv.at[s],
            device_id={"coil": lax.rem(j + s, GRP)},
            device_id_type=MESH,
        )
        c.start()
        acopy.append(c)

    loads[7].wait()
    loads[8].wait()

    def columns(shifts):
        for s in shifts:
            rq = pl.multiple_of(lax.rem(j - s + GRP, GRP) * RB, RB)
            xv = xb[pl.ds(rq, RB), :].astype(F32)
            x_re, x_im = xv[:, :N], xv[:, N:]
            for c in range(NCO):
                sv = sens[c, pl.ds(rq, RB), :].astype(F32)
                s_re, s_im = sv[:, :N], sv[:, N:]
                ci[s, c * RB : (c + 1) * RB, :N] = (s_re * x_re - s_im * x_im).astype(BF16)
                ci[s, c * RB : (c + 1) * RB, N:] = (s_re * x_im + s_im * x_re).astype(BF16)
        for s in shifts:
            rq = pl.multiple_of(lax.rem(j - s + GRP, GRP) * RB, RB)
            for half in range(2):
                spec = dot(ci[s], table[0, :, half * N : (half + 1) * N]).astype(BF16)
                for c in range(NCO):
                    cols[c, pl.ds(half * ROWS + rq, RB), :] = spec[c * RB : (c + 1) * RB]

    columns((0,))
    for shifts in ((4, 1, 7), (3, 5), (2, 6)):
        for s in shifts:
            pltpu.make_async_remote_copy(
                src_ref=xb.at[pl.ds(r0, RB)],
                dst_ref=xb.at[pl.ds(pl.multiple_of(lax.rem(j - s + GRP, GRP) * RB, RB), RB)],
                send_sem=asend.at[s],
                recv_sem=arecv.at[s],
                device_id={"coil": lax.rem(j + s, GRP)},
                device_id_type=MESH,
            ).wait_recv()
        columns(shifts)

    loads[9].wait()
    loads[10].wait()

    for c in range(NCO):
        for half in range(2):
            est = dot(table[1, half * ROWS : (half + 1) * ROWS, :], cols[c])
            k = ksp[c, :, half * N : (half + 1) * N].astype(F32)
            misfit[c, :, half * N : (half + 1) * N] = (est - k).astype(BF16)
    for c in range(NCO):
        for half in range(2):
            stacked[c, half * ROWS : (half + 1) * ROWS, :] = dot(
                misfit[c], table[1, :, half * N : (half + 1) * N]
            ).astype(BF16)
    def gradient(base):
        base = pl.multiple_of(base, 128)
        rows = pl.ds(base, 128)
        into = pl.ds(base + 8, 128)
        for c in range(NCO):
            m = mask[c : c + 1, :].astype(F32).astype(BF16)
            mm = jnp.concatenate([m, m], axis=1)
            b_re = dot(table[0, rows, :] * mm, stacked[c])
            b_im = dot(table[0, pl.ds(base + ROWS, 128), :] * mm, stacked[c])
            s_re, s_im = sens[c, rows, :N].astype(F32), sens[c, rows, N:].astype(F32)
            g_re = s_re * b_re + s_im * b_im
            g_im = s_re * b_im - s_im * b_re
            acc[into, :N] = g_re if c == 0 else acc[into, :N] + g_re
            acc[into, N:] = g_im if c == 0 else acc[into, N:] + g_im

    def haloed(q):
        v = acc[pl.ds(pl.multiple_of(q * RB, RB), HR + 8), :][5 : 5 + HR]
        return jnp.concatenate([v[:, :N], v[:, N:]], axis=0)

    bcopy = []

    def send(targets):
        begun = []
        for to in targets:
            slot = len(bcopy) + len(begun)
            gs[slot] = haloed(to).astype(BF16)
            s = lax.rem(to - j + GRP, GRP)
            begun.append(
                pltpu.make_async_remote_copy(
                    src_ref=gs.at[slot],
                    dst_ref=grecv.at[s],
                    send_sem=bsend.at[s],
                    recv_sem=brecv.at[s],
                    device_id={"coil": to},
                    device_id_type=MESH,
                )
            )
            if len(begun) > 1:
                begun[-2].start()
        begun[-1].start()
        bcopy.extend(begun)

    low = j < GRP // 2
    acc[:8, :] = jnp.zeros((8, 2 * N), F32)
    acc[ROWS + 8 :, :] = jnp.zeros((8, 2 * N), F32)
    gradient(jnp.where(low, 128, 0))
    send([jnp.where(low, 5, 0) + n for n in range(3)])
    gradient(jnp.where(low, 0, 128))
    start = jnp.where(low, 0, 3)
    send([start + lax.rem(j - start + n, 5) for n in range(1, 5)])

    xr[:ROWS, :] = pltpu.roll(xb[...].astype(F32), 3, axis=0)
    xr[ROWS:, :] = jnp.zeros((16, 2 * N), F32)
    for half in range(2):
        cut = slice(half * N, (half + 1) * N)
        xh[half * HR : (half + 1) * HR, :] = xr[pl.ds(r0, HR), cut]
        xh[half * HR + 3 : half * HR + 3 + RB, :] = image[:, cut]
    total = xh[...] - haloed(j)
    bias1, bias2 = other_weights(pick, wm, wl, bf, bm, w54, w2, w3)
    for s in (4, 3, 5, 2, 6, 1, 7):
        pltpu.make_async_remote_copy(
            src_ref=gs.at[0],
            dst_ref=grecv.at[s],
            send_sem=bsend.at[s],
            recv_sem=brecv.at[s],
            device_id={"coil": lax.rem(j + s, GRP)},
            device_id_type=MESH,
        ).wait_recv()
        total = total - grecv[s].astype(F32)
    line = lax.broadcasted_iota(jnp.int32, (2 * HR, N), 0)
    row = r0 - 3 + jnp.where(line >= HR, line - HR, line)
    total = jnp.where((row >= 0) & (row < ROWS), total, 0.0)
    xh[...] = total
    hb[2] = total.astype(BF16)

    for d, here in partners:
        def ccopy(d=d):
            return pltpu.make_async_remote_copy(
                src_ref=hb.at[2],
                dst_ref=hb.at[2 - d],
                send_sem=csend.at[d + 2],
                recv_sem=crecv.at[d + 2],
                device_id={"frame": t + d},
                device_id_type=MESH,
            )

        @pl.when(here)
        def _():
            ccopy().start()

        @pl.when(jnp.logical_not(here))
        def _():
            hb[2 + d] = jnp.zeros((2 * HR, N), BF16)

    def planes(f):
        v = hb[f].astype(F32)
        parts = []
        for half in range(2):
            p = v[half * HR : (half + 1) * HR]
            parts += [shift_right(p), p, shift_left(p)]
        for i in range(HR // 8):
            kb[i, f * KF : (f + 1) * KF, :] = jnp.concatenate(
                [p[8 * i : 8 * i + 8] for p in parts], axis=0
            ).astype(BF16)

    def arrived(d):
        @pl.when((t + d >= 0) & (t + d < frames))
        def _():
            pltpu.make_async_remote_copy(
                src_ref=hb.at[2],
                dst_ref=hb.at[2 + d],
                send_sem=csend.at[2 - d],
                recv_sem=crecv.at[2 - d],
                device_id={"frame": t + d},
                device_id_type=MESH,
            ).wait_recv()

        planes(2 + d)

    def first(f):
        def put(q, v):
            h1[f, q * CH : (q + 1) * CH, :] = jnp.maximum(v + bias1, 0.0).astype(BF16)

        for i in range(5):
            here_k = kb[i, f * KF : (f + 3) * KF, :]
            if i == 4:
                top = dot(w1[: 4 * CH, :], here_k)
                for q in range(4):
                    put(32 + q, top[q * CH : (q + 1) * CH])
                continue
            next_k = kb[i + 1, f * KF : (f + 3) * KF, :]
            top = dot(w1[: 6 * CH, :], here_k)
            low = dot(w1[6 * CH : 8 * CH, :], here_k) + dot(w1[8 * CH :, :], next_k)
            for q in range(6):
                put(8 * i + q, top[q * CH : (q + 1) * CH])
            for q in range(2):
                put(8 * i + 6 + q, low[q * CH : (q + 1) * CH])

    planes(2)
    arrived(-1)
    arrived(1)
    first(1)
    arrived(-2)
    first(0)
    arrived(2)
    first(2)

    @pl.when(j == 0)
    def _():
        h1[:, : 2 * CH, :] = jnp.zeros((3, 2 * CH, N), BF16)

    @pl.when(j == GRP - 1)
    def _():
        h1[:, 34 * CH :, :] = jnp.zeros((3, 2 * CH, N), BF16)

    @pl.when(t == 0)
    def _():
        h1[0] = jnp.zeros((36 * CH, N), BF16)

    @pl.when(t == frames - 1)
    def _():
        h1[2] = jnp.zeros((36 * CH, N), BF16)

    for r in range(34):
        base = r * CH
        taps = dot(w2[0], h1[0, base : base + 3 * CH, :])
        taps += dot(w2[1], h1[1, base : base + 3 * CH, :])
        taps += dot(w2[2], h1[2, base : base + 3 * CH, :])
        v = taps[CH : 2 * CH] + shift_right(taps[:CH]) + shift_left(taps[2 * CH :]) + bias2
        h2[base : base + CH, :] = jnp.maximum(v, 0.0).astype(BF16)

    @pl.when(j == 0)
    def _():
        h2[:CH, :] = jnp.zeros((CH, N), BF16)

    @pl.when(j == GRP - 1)
    def _():
        h2[33 * CH :, :] = jnp.zeros((CH, N), BF16)

    blocks = []
    for i in range(RB // 8):
        base = i * 8 * CH
        taps = dot(w3[...], h2[base : base + 10 * CH, :])
        blocks.append(taps[48:96] + shift_right(taps[:48]) + shift_left(taps[96:]))
    for a in (0, 2, 1):
        for half in range(2):
            o = (a * 2 + half) * 8
            v = jnp.concatenate([b[o : o + 8] for b in blocks], axis=0)
            cut = slice(half * N, (half + 1) * N)
            if a == 1:
                xh[half * HR + 3 : half * HR + 3 + RB, :] += v
            else:
                psend[a // 2, :, cut] = v.astype(BF16)

    ends = [(1, 0, t + 1 < frames), (-1, 1, t >= 1)]
    for n, (d, a, here) in enumerate(ends):
        @pl.when(here)
        def _():
            pltpu.make_async_remote_copy(
                src_ref=psend.at[a],
                dst_ref=precv.at[n],
                send_sem=dsend.at[n],
                recv_sem=drecv.at[n],
                device_id={"frame": t + d},
                device_id_type=MESH,
            ).start()

    for half in range(2):
        out_ref[:, half * N : (half + 1) * N] = xh[half * HR + 3 : half * HR + 3 + RB, :]
    for n, (d, a, here) in enumerate(ends):
        @pl.when((t - d >= 0) & (t - d < frames))
        def _():
            pltpu.make_async_remote_copy(
                src_ref=psend.at[a],
                dst_ref=precv.at[n],
                send_sem=dsend.at[n],
                recv_sem=drecv.at[n],
                device_id={"frame": t - d},
                device_id_type=MESH,
            ).wait_recv()
            out_ref[...] += precv[n].astype(F32)

    for c in acopy + bcopy:
        c.wait_send()
    for d, here in partners:
        @pl.when(here)
        def _():
            pltpu.make_async_remote_copy(
                src_ref=hb.at[2],
                dst_ref=hb.at[2 - d],
                send_sem=csend.at[d + 2],
                recv_sem=crecv.at[d + 2],
                device_id={"frame": t + d},
                device_id_type=MESH,
            ).wait_send()
    for n, (d, a, here) in enumerate(ends):
        @pl.when(here)
        def _():
            pltpu.make_async_remote_copy(
                src_ref=psend.at[a],
                dst_ref=precv.at[n],
                send_sem=dsend.at[n],
                recv_sem=drecv.at[n],
                device_id={"frame": t + d},
                device_id_type=MESH,
            ).wait_send()


def picks():
    out = np.zeros((6, 144, 64), np.float32)
    for b in range(3):
        for k in range(18):
            a, ch, e = k // 6, k // 3 % 2, k % 3
            out[b, 8 * k : 8 * k + 8, ((a * 3 + b) * 3 + e) * 2 + ch] = 1
            e, a, ch = k // 6, k // 2 % 3, k % 2
            out[3 + b, 8 * k : 8 * k + 8, ((a * 3 + b) * 3 + e) * 2 + ch] = 1
    return out


def shards(frames, kspace, sens, mask, image, w_first, b_first, w_mid, b_mid, w_last):
    args = (
        kspace[0], sens, mask[0], image[0], jnp.asarray(dft_tables(), BF16), jnp.asarray(picks(), BF16),
        jnp.swapaxes(w_first, 3, 4).reshape(27, 2, CH), w_mid.reshape(27, CH, CH), w_last.reshape(27, 2, CH),
        b_first[None], b_mid[None],
    )
    dma = pltpu.SemaphoreType.DMA
    out = pl.pallas_call(
        functools.partial(kernel, frames),
        out_shape=pltpu.VMEM((RB, 2 * N), F32),
        in_specs=[pl.BlockSpec(memory_space=pl.ANY)] * len(args),
        out_specs=pl.BlockSpec(memory_space=pltpu.VMEM),
        scratch_shapes=[pltpu.VMEM(a.shape, a.dtype) for a in args]
        + [
            pltpu.VMEM((64, CH), F32),
            pltpu.VMEM((640, 144), BF16),
            pltpu.VMEM((3, 3 * CH, 3 * CH), BF16),
            pltpu.VMEM((144, 640), BF16),
            pltpu.VMEM((ROWS, 2 * N), BF16),
            pltpu.VMEM((GRP, NCO * RB, 2 * N), BF16),
            pltpu.VMEM((NCO, 2 * ROWS, N), BF16),
            pltpu.VMEM((NCO, ROWS, 2 * N), BF16),
            pltpu.VMEM((NCO, 2 * ROWS, N), BF16),
            pltpu.VMEM((ROWS + 16, 2 * N), F32),
            pltpu.VMEM((GRP, 2 * HR, N), BF16),
            pltpu.VMEM((GRP, 2 * HR, N), BF16),
            pltpu.VMEM((ROWS + 16, 2 * N), F32),
            pltpu.VMEM((2 * HR, N), F32),
            pltpu.VMEM((5, 2 * HR, N), BF16),
            pltpu.VMEM((HR // 8, 5 * KF, N), BF16),
            pltpu.VMEM((3, 36 * CH, N), BF16),
            pltpu.VMEM((34 * CH, N), BF16),
            pltpu.VMEM((2, RB, 2 * N), BF16),
            pltpu.VMEM((2, RB, 2 * N), BF16),
            dma((len(args),)), dma((GRP,)), dma((GRP,)), dma((GRP,)), dma((GRP,)),
            dma((5,)), dma((5,)), dma((2,)), dma((2,)),
        ],
        compiler_params=pltpu.CompilerParams(
            collective_id=0, has_side_effects=True, vmem_limit_bytes=56 * 1024 * 1024
        ),
    )(*args)
    return out[None]


def solution(mesh):
    in_specs = (
        P("frame", "coil", None, None),
        P("coil", None, None),
        P("frame", "coil", None),
        P("frame", "coil", None),
        P(),
        P(),
        P(),
        P(),
        P(),
    )
    out_specs = P("frame", "coil", None)
    body = functools.partial(shards, mesh.shape["frame"])
    return jax.shard_map(body, mesh=mesh, in_specs=in_specs, out_specs=out_specs, check_vma=False)
```
